256 devices in a mesh: tm: 16 (over z, core), space: 16 (over x, y).
Axes of the slice: x: 4, y: 4, z: 8, core: 2. Of those that a mesh axis runs over, the one named last changes fastest.
Arguments:
- slab_starts: float32 [16, 4, 4, 4, 128, 128], P('tm', None, None, None, 'space'), may hold values from -1.4 to 6, as said below
- coarse_factor: float32 [4, 128, 128], P(None, 'space'), may hold values from 0.2 to 1
- blend_weight: float32 [128, 128], P('space'), may hold values from 0.2 to 0.9
- blend_flags: int32 [128, 128], P('space'), may hold values 0 or 1
Outputs:
- slab_ends: float32 [16, 4, 4, 4, 128, 128], P('tm', None, None, None, 'space')
- jump_norm: float32 [16], P('tm')
The draws below stay inside these ranges and needn't reach their ends.
Inputs may be any that keep to these rules, and one draw needn't show every extreme that they name: `slab_starts`: at every node the density and the pressure lie between 0.5 and 2 and each velocity component between -0.7 and 0.7.
All inputs are finite; a program needn't handle non-finite values. No bound on the sum of `blend_flags` on one device may be relied on, other than what follows from the above.
Results may differ from the reference program's by a relative error of at most 0.0003.
Values sent between devices are 32-bit elements; how exact they have to be, the bound alone decides.
No kernel may reach another device: no remote copies, remote signals or barrier semaphores. Data moves between devices by JAX's collectives and lax.ppermute only.
A program may use at most 128 MiB of HBM per device.

```python
import math
import jax
import jax.numpy as jnp
import numpy as np
from jax import lax

VARS = 4
NODES = 4
FSTEPS = 4
EY = 128
SLABS = 16
NX = 128


def draw_slab_starts(key, part):
    grid_shape = (SLABS, NODES, NODES, NX, EY)
    subkeys = jax.random.split(jax.random.fold_in(key, 17), 4)
    density = jnp.exp(jax.random.uniform(subkeys[0], grid_shape, jnp.float32, math.log(0.5), math.log(2.0)))
    pressure = jnp.exp(jax.random.uniform(subkeys[1], grid_shape, jnp.float32, math.log(0.5), math.log(2.0)))
    velocity_x = jnp.clip(0.3 * jax.random.normal(subkeys[2], grid_shape, jnp.float32), -0.7, 0.7)
    velocity_y = jnp.clip(0.3 * jax.random.normal(subkeys[3], grid_shape, jnp.float32), -0.7, 0.7)
    energy = pressure / 0.4 + 0.5 * density * (velocity_x * velocity_x + velocity_y * velocity_y)
    return jnp.stack([density, density * velocity_x, density * velocity_y, energy], axis=1)


def place_ends(result, key, low, top_value):
    longest = result.shape.index(max(result.shape))
    spots = []
    for shift in (0, 1):
        where = [jax.random.randint(jax.random.fold_in(key, axis), (), 0, length) for axis, length in enumerate(result.shape)]
        where[longest] = (where[longest] + shift) % result.shape[longest]
        spots.append(tuple(where))
    return result.at[spots[0]].set(low).at[spots[1]].set(top_value)


def level_of(stream_key, shape, pieces, low, high):
    level = 1.0
    for axis_at, parts in pieces:
        heights = jax.random.uniform(jax.random.fold_in(jax.random.fold_in(stream_key, 6), axis_at), (parts,), jnp.float32, low / len(pieces), high / len(pieces))
        level = level * jnp.repeat(jnp.exp(heights), shape[axis_at] // parts).reshape((-1,) + (1,) * (len(shape) - 1 - axis_at))
    return level


def setup_inputs(seed: int = 0) -> dict:
    arg_keys = jax.random.split(jax.random.key(seed), 5)
    slab_starts = draw_slab_starts(jax.random.fold_in(arg_keys[4], 71), 0)
    coarse_factor = jnp.clip(jnp.exp(math.log(1.0) - 1.609438 * jax.random.uniform(arg_keys[1], (VARS, NX, EY), jnp.float32) ** level_of(arg_keys[1], (VARS, NX, EY), ((1, 16),), -0.2, 0.2)), 0.2, 1.0)
    blend_weight = jnp.clip(0.2 + 0.7 * jax.random.uniform(arg_keys[2], (NX, EY), jnp.float32) ** level_of(arg_keys[2], (NX, EY), ((0, 16),), -0.2, 0.2), 0.2, 0.9)
    blend_flags = place_ends((jax.random.randint(arg_keys[3], (NX, EY), 0, 2) < 1).astype(jnp.int32), jax.random.fold_in(arg_keys[3], 1), 0, 1)
    return {"slab_starts": slab_starts, "coarse_factor": coarse_factor, "blend_weight": blend_weight, "blend_flags": blend_flags}


gamma_ratio = 1.4
step_size = 0.003

def tables():
    inner = 1.0 / math.sqrt(5.0)
    points = np.array([-1.0, -inner, inner, 1.0])
    weights = np.array([1.0 / 6.0, 5.0 / 6.0, 5.0 / 6.0, 1.0 / 6.0])
    scales = np.array([1.0 / np.prod([points[column] - points[others] for others in range(4) if others != column]) for column in range(4)])
    derivative = np.zeros((4, 4))
    for row_index in range(4):
        for col_index in range(4):
            if row_index != col_index:
                derivative[row_index, col_index] = scales[col_index] / scales[row_index] / (points[row_index] - points[col_index])
        derivative[row_index, row_index] = -np.sum(derivative[row_index])
    return (jnp.asarray(derivative, dtype=jnp.float32), jnp.asarray(weights, dtype=jnp.float32))

def primitives(state):
    density = state[0]
    velocity_x = state[1] / density
    velocity_y = state[2] / density
    pressure = (gamma_ratio - 1.0) * (state[3] - 0.5 * density * (velocity_x * velocity_x + velocity_y * velocity_y))
    return (density, velocity_x, velocity_y, pressure)

def log_terms(left, right):
    ratio = (left * (left - 2.0 * right) + right * right) / (left * (left + 2.0 * right) + right * right)
    series = 105.0 + ratio * (35.0 + ratio * (21.0 + ratio * 15.0))
    nearly = ratio < 0.0001
    safe_left = jnp.where(nearly, 1.0, left)
    safe_right = jnp.where(nearly, 2.0, right)
    return (nearly, series, jnp.log(safe_right / safe_left), safe_right - safe_left)

def log_mean(left, right):
    nearly, series, logged, differ = log_terms(left, right)
    return jnp.where(nearly, (left + right) * 52.5 / series, differ / logged)

def inverse_log_mean(left, right):
    nearly, series, logged, differ = log_terms(left, right)
    return jnp.where(nearly, series / (52.5 * (left + right)), logged / differ)

def entropy_flux(left, right):
    density_left, normal_left, along_left, pressure_left = left
    density_right, normal_right, along_right, pressure_right = right
    mass_mean = log_mean(density_left, density_right)
    normal_mean = 0.5 * (normal_left + normal_right)
    along_mean = 0.5 * (along_left + along_right)
    pressure_mean = 0.5 * (pressure_left + pressure_right)
    thermal = pressure_left * pressure_right * inverse_log_mean(density_left * pressure_right, density_right * pressure_left)
    kinetic = 0.5 * (normal_left * normal_right + along_left * along_right)
    mass_flux = mass_mean * normal_mean
    normal_flux = mass_flux * normal_mean + pressure_mean
    along_flux = mass_flux * along_mean
    energy_flux = mass_flux * (kinetic + thermal / (gamma_ratio - 1.0)) + 0.5 * (pressure_left * normal_right + pressure_right * normal_left)
    return (mass_flux, normal_flux, along_flux, energy_flux)

def physical_flux(prims):
    density, normal, along, pressure = prims
    mass_flux = density * normal
    energy_total = pressure / (gamma_ratio - 1.0) + 0.5 * density * (normal * normal + along * along)
    return (mass_flux, mass_flux * normal + pressure, mass_flux * along, normal * (energy_total + pressure))

def oriented(prims, axis):
    density, velocity_x, velocity_y, pressure = prims
    if axis == 1:
        return (density, velocity_x, velocity_y, pressure)
    return (density, velocity_y, velocity_x, pressure)

def restack(fluxes, axis):
    mass_flux, normal_flux, along_flux, energy_flux = fluxes
    if axis == 1:
        return jnp.stack([mass_flux, normal_flux, along_flux, energy_flux], 0)
    return jnp.stack([mass_flux, along_flux, normal_flux, energy_flux], 0)

def wave_speed(prims):
    density, normal, along, pressure = prims
    return jnp.abs(normal) + jnp.sqrt(gamma_ratio * pressure / density)

def rusanov(state_left, state_right, axis, central):
    prims_left = oriented(primitives(state_left), axis)
    prims_right = oriented(primitives(state_right), axis)
    if central:
        centre = restack(entropy_flux(prims_left, prims_right), axis)
    else:
        centre = 0.5 * (restack(physical_flux(prims_left), axis) + restack(physical_flux(prims_right), axis))
    speed = jnp.maximum(wave_speed(prims_left), wave_speed(prims_right))
    return centre - 0.5 * speed * (state_right - state_left)

def direction_rate(state, axis, face_left, face_right, blend, derivative, weights):
    prims = oriented(primitives(state), axis)
    node = axis - 1
    rows = tuple((jnp.expand_dims(field, node + 1) for field in prims))
    columns = tuple((jnp.expand_dims(field, node) for field in prims))
    pairs = restack(entropy_flux(rows, columns), axis)
    table_shape = [1, 1, 1, 1, 1, 1]
    table_shape[axis] = 4
    table_shape[axis + 1] = 4
    volume = lax.optimization_barrier(jnp.sum((2.0 * derivative).reshape(table_shape) * pairs, axis=axis + 1))
    physical = restack(physical_flux(prims), axis)
    lower = (face_left - jnp.take(physical, 0, axis=axis)) / weights[0]
    upper = (face_right - jnp.take(physical, 3, axis=axis)) / weights[3]
    middle = jnp.zeros_like(lax.slice_in_dim(physical, 1, 3, axis=axis))
    boundary = jnp.concatenate([-jnp.expand_dims(lower, axis), middle, jnp.expand_dims(upper, axis)], axis)
    galerkin = -2.0 * (volume + boundary)
    inner_flux = rusanov(lax.slice_in_dim(state, 0, 3, axis=axis), lax.slice_in_dim(state, 1, 4, axis=axis), axis, False)
    walls = jnp.concatenate([jnp.expand_dims(face_left, axis), inner_flux, jnp.expand_dims(face_right, axis)], axis)
    weight_shape = [1, 1, 1, 1, 1]
    weight_shape[axis] = 4
    subcell = -2.0 * (lax.slice_in_dim(walls, 1, 5, axis=axis) - lax.slice_in_dim(walls, 0, 4, axis=axis)) / weights.reshape(weight_shape)
    return (1.0 - blend) * galerkin + blend * subcell

def vertical_faces(state):
    lower_trace = state[:, :, 0]
    upper_trace = state[:, :, 3]
    behind = jnp.roll(upper_trace, 1, axis=3)
    face_left = rusanov(behind, lower_trace, 2, True)
    return (face_left, jnp.roll(face_left, -1, axis=3))

def rolled_faces(state):
    lower_trace = state[:, 0]
    upper_trace = state[:, 3]
    behind = jnp.roll(upper_trace, 1, axis=2)
    face_left = rusanov(behind, lower_trace, 1, True)
    return (face_left, jnp.roll(face_left, -1, axis=2))

def rate(state, blend, derivative, weights, horizontal):
    face_left, face_right = horizontal(state)
    across = direction_rate(state, 1, face_left, face_right, blend, derivative, weights)
    face_low, face_high = vertical_faces(state)
    upward = direction_rate(state, 2, face_low, face_high, blend, derivative, weights)
    return across + upward

def fine_slab(state, blend, derivative, weights, horizontal):
    for repeat_index in range(FSTEPS):
        section = state + step_size * rate(state, blend, derivative, weights, horizontal)
        state = 0.5 * state + 0.5 * (section + step_size * rate(section, blend, derivative, weights, horizontal))
    return state

def quadrature_table(weights):
    return (weights[:, None] * weights[None, :] / 4.0).reshape(1, 4, 4, 1, 1)

def coarse(state, factor, quadrature):
    average = lax.optimization_barrier(jnp.sum(state * quadrature, axis=(1, 2), keepdims=True))
    return average + factor * (state - average)

def reference(slab_starts, coarse_factor, blend_weight, blend_flags):
    derivative, weights = tables()
    quadrature = quadrature_table(weights)
    blend = blend_flags.astype(jnp.float32) * blend_weight
    factor = coarse_factor[:, None, None]

    def advance_fine(opening):
        return fine_slab(opening, blend, derivative, weights, rolled_faces)
    fine_ends = lax.map(advance_fine, slab_starts)
    corrections = fine_ends - jax.vmap(lambda opening: coarse(opening, factor, quadrature))(slab_starts)

    def advance(carried, correction):
        closing = coarse(carried, factor, quadrature) + correction
        return (closing, (carried, closing))
    unused, (new_starts, slab_ends) = lax.scan(advance, slab_starts[0], corrections)
    jumps = new_starts - slab_starts
    totals = lax.optimization_barrier(jnp.sum(quadrature[None] * jumps * jumps, axis=(1, 2, 3, 4, 5)))
    jump_norm = jnp.sqrt(totals / (NX * EY))
    return (slab_ends, jump_norm)
```

```python
import math

import jax
import jax.numpy as jnp
import numpy as np
from jax import lax
from jax.experimental import pallas as pl
from jax.experimental.pallas import tpu as pltpu
from jax.sharding import Mesh
from jax.sharding import PartitionSpec as P

FSTEPS = 4
SPACE = ("space_0", "space_1")
TM = ("tm_0", "tm_1")
STEP = 0.003
WEIGHTS = (1.0 / 6.0, 5.0 / 6.0, 5.0 / 6.0, 1.0 / 6.0)
ROWS = 32


def derivative_table():
    inner = 1.0 / math.sqrt(5.0)
    points = np.array([-1.0, -inner, inner, 1.0])
    scales = np.array(
        [1.0 / np.prod([points[c] - points[o] for o in range(4) if o != c]) for c in range(4)]
    )
    table = np.zeros((4, 4))
    for r in range(4):
        for c in range(4):
            if r != c:
                table[r, c] = scales[c] / scales[r] / (points[r] - points[c])
        table[r, r] = -np.sum(table[r])
    return table


SPLIT = [[float(2.0 * WEIGHTS[i] * derivative_table()[i, k]) for k in range(4)] for i in range(4)]
SERIES = (105.0 / 52.5, 35.0 / 52.5, 21.0 / 52.5, 15.0 / 52.5)


def log_parts(left, right, log_left, log_right):
    total = left + right
    differ = right - left
    ratio = differ / total
    ratio = ratio * ratio
    nearly = ratio < 0.0001
    series = SERIES[0] + ratio * (SERIES[1] + ratio * (SERIES[2] + ratio * SERIES[3]))
    return jnp.where(nearly, total, differ), jnp.where(nearly, series, log_right - log_left)


def pair_flux(a, b, scale=None):
    top, bottom = log_parts(a["rho"], b["rho"], a["lrho"], b["lrho"])
    mean = top / bottom
    top, bottom = log_parts(a["beta"], b["beta"], a["lbeta"], b["lbeta"])
    thermal = bottom / top
    normal = a["n"] + b["n"]
    pressure = a["p"] + b["p"]
    cross = a["p"] * b["n"] + b["p"] * a["n"]
    if scale is not None:
        mean = mean * scale
        pressure = pressure * scale
        cross = cross * scale
    mass = mean * normal
    half = 0.5 * mass
    kinetic = a["n"] * b["n"] + a["t"] * b["t"] + thermal
    return (
        mass,
        half * normal + pressure,
        half * (a["t"] + b["t"]),
        half * kinetic + cross,
    )


def conserved(node):
    return (node["rho"], node["mn"], node["mt"], node["e"])


def face_flux(a, b):
    central = pair_flux(a, b)
    speed = jnp.maximum(jnp.abs(a["n"]) + a["c"], jnp.abs(b["n"]) + b["c"])
    return tuple(
        c - speed * (ub - ua) for c, ua, ub in zip(central, conserved(a), conserved(b), strict=True)
    )


def physical(node):
    return (
        node["mn"],
        node["mn"] * node["n"] + node["p"],
        node["mt"] * node["n"],
        node["n"] * (node["e"] + node["p"]),
    )


def line_walls(nodes, blend):
    walls = [None, None, None]
    for i in range(4):
        for k in range(i + 1, 4):
            flux = pair_flux(nodes[i], nodes[k], SPLIT[i][k])
            for m in range(i, k):
                walls[m] = (
                    flux
                    if walls[m] is None
                    else tuple(x + y for x, y in zip(walls[m], flux, strict=True))
                )
    own = [physical(node) for node in nodes]
    speeds = [jnp.abs(node["n"]) + node["c"] for node in nodes]
    out = []
    for m in range(3):
        speed = jnp.maximum(speeds[m], speeds[m + 1])
        ua, ub = conserved(nodes[m]), conserved(nodes[m + 1])
        merged = []
        for v in range(4):
            sub = own[m][v] + own[m + 1][v] - speed * (ub[v] - ua[v])
            merged.append(walls[m][v] + blend * (sub - walls[m][v]))
        out.append(merged)
    return out


ORDER = {1: (0, 1, 2, 3), 2: (0, 2, 1, 3)}
VX, VY, PR, LR, BE, LB, CS = range(7)


def at(v, i, j):
    return v * 16 + i * 4 + j


def fine_kernel(
    slab_ref, own_ref, left_ref, right_ref, factor_ref, packed_ref, plain_ref,
    base, mid, blend_ref, prim, faces,
):
    def copy_in(k, carry):
        base[k, 0:8, :] = left_ref[k]
        base[k, 8:16, :] = own_ref[k]
        base[k, 16:24, :] = right_ref[k]
        return carry

    lax.fori_loop(0, 64, copy_in, 0, unroll=8)
    blend_ref[0:8, :] = left_ref[64]
    blend_ref[8:16, :] = own_ref[64]
    blend_ref[16:24, :] = right_ref[64]
    blend_ref[24:32, :] = jnp.zeros((8, 128), jnp.float32)

    def rows(c, offset):
        return pl.ds(pl.multiple_of(c * 8, 8) + offset, 8)

    def node_pass(src, c):
        here = rows(c, 0)
        for n in range(16):
            rho = src[n, here, :]
            inv = 1.0 / rho
            vx = src[16 + n, here, :] * inv
            vy = src[32 + n, here, :] * inv
            p = 0.4 * (src[48 + n, here, :] - 0.5 * rho * (vx * vx + vy * vy))
            beta = 0.2 * rho / p
            prim[VX * 16 + n, here, :] = vx
            prim[VY * 16 + n, here, :] = vy
            prim[PR * 16 + n, here, :] = p
            prim[LR * 16 + n, here, :] = jnp.log(rho)
            prim[BE * 16 + n, here, :] = beta
            prim[LB * 16 + n, here, :] = jnp.log(beta)
            prim[CS * 16 + n, here, :] = jnp.sqrt(1.4 * p * inv)

    def node(src, i, j, here, axis):
        n = i * 4 + j
        normal, along = (VX, VY) if axis == 1 else (VY, VX)
        order = ORDER[axis]
        return {
            "rho": src[n, here, :],
            "mn": src[order[1] * 16 + n, here, :],
            "mt": src[order[2] * 16 + n, here, :],
            "e": src[48 + n, here, :],
            "n": prim[normal * 16 + n, here, :],
            "t": prim[along * 16 + n, here, :],
            "p": prim[PR * 16 + n, here, :],
            "lrho": prim[LR * 16 + n, here, :],
            "beta": prim[BE * 16 + n, here, :],
            "lbeta": prim[LB * 16 + n, here, :],
            "c": prim[CS * 16 + n, here, :],
        }

    def face_pass(src, c):
        for j in range(4):
            flux = face_flux(node(src, 3, j, rows(c, 0), 1), node(src, 0, j, rows(c, 1), 1))
            for v in range(4):
                faces[j * 4 + v, rows(c, 0), :] = flux[v]

    def update_pass(src, dst, c, second):
        here = rows(c, 1)
        blend = blend_ref[rows(c, 0), :]
        share = 0.5 if second else 1.0
        for j in range(4):
            walls = line_walls([node(src, i, j, here, 1) for i in range(4)], blend)
            for v in range(4):
                column = [faces[j * 4 + v, rows(c, 0), :]]
                column += [walls[m][v] for m in range(3)]
                column += [faces[j * 4 + v, here, :]]
                for i in range(4):
                    k = at(v, i, j)
                    change = (share * STEP / WEIGHTS[i]) * (column[i + 1] - column[i])
                    if second:
                        start = 0.5 * (dst[k, rows(c, 2), :] + src[k, here, :])
                    else:
                        start = src[k, here, :]
                    dst[k, rows(c, 0), :] = start - change
        for i in range(4):
            nodes = [node(src, i, j, here, 2) for j in range(4)]
            behind = {key: pltpu.roll(x, 1, 1) for key, x in nodes[3].items()}
            low = face_flux(behind, nodes[0])
            high = tuple(pltpu.roll(x, 127, 1) for x in low)
            walls = line_walls(nodes, blend)
            for q in range(4):
                v = ORDER[2][q]
                column = [low[q]] + [walls[m][q] for m in range(3)] + [high[q]]
                for j in range(4):
                    k = at(v, i, j)
                    change = (share * STEP / WEIGHTS[j]) * (column[j + 1] - column[j])
                    dst[k, rows(c, 0), :] = dst[k, rows(c, 0), :] - change

    def stage(src, dst, s, second):
        for c in range(3):
            blend_ref[8 * c : 8 * c + 8, :] = blend_ref[8 * c + 1 : 8 * c + 9, :]

        def run(body, count):
            def step(c, carry):
                body(c)
                return carry

            lax.fori_loop(0, lax.shift_right_logical(count - 2 * s, 3), step, 0)

        run(lambda c: node_pass(src, c), 31)
        run(lambda c: face_pass(src, c), 30)
        run(lambda c: update_pass(src, dst, c, second), 29)

    def time_step(t, carry):
        stage(base, mid, 2 * t, False)
        stage(mid, base, 2 * t + 1, True)
        return carry

    lax.fori_loop(0, FSTEPS, time_step, 0)

    later = jnp.where(slab_ref[0] == 0, 0.0, 1.0).astype(jnp.float32)
    for v in range(4):
        factor = factor_ref[v]
        mean = weighted_mean([own_ref[v * 16 + n] for n in range(16)])
        for i in range(4):
            kept = []
            for j in range(4):
                k = at(v, i, j)
                guess = mean + factor * (own_ref[k] - mean)
                kept.append(base[k, 0:8, :] - later * guess)
                plain_ref[k] = kept[j]
            for q, piece in enumerate(exchange(kept)):
                packed_ref[v * 4 + q, i] = piece


def weighted_mean(values):
    total = None
    for n, x in enumerate(values):
        term = (WEIGHTS[n // 4] * WEIGHTS[n % 4] / 4.0) * x
        total = term if total is None else total + term
    return total


def exchange(blocks):
    group = lax.broadcasted_iota(jnp.int32, (8, 128), 0) // 2
    out = []
    for q in range(4):
        piece = None
        for j in range(4):
            shift = (2 * (j - q)) % 8
            moved = pltpu.roll(blocks[j], shift, 0) if shift else blocks[j]
            piece = moved if piece is None else jnp.where(group == j, moved, piece)
        out.append(piece)
    return out


def scan_kernel(slab_ref, given_ref, factor_ref, out_ref):
    slab = slab_ref[0]
    var = lax.shift_right_logical(slab, 2)
    first = 2 * (slab & 3)
    row = lax.broadcasted_iota(jnp.int32, (8, 128), 0)
    even = jnp.broadcast_to(factor_ref[var, pl.ds(first, 1), :], (8, 128))
    odd = jnp.broadcast_to(factor_ref[var, pl.ds(first + 1, 1), :], (8, 128))
    factor = jnp.where((row & 1) == 0, even, odd)
    outer = (row < 2) | (row >= 6)
    low = jnp.where(outer, WEIGHTS[0], WEIGHTS[1]).astype(jnp.float32) * (WEIGHTS[0] / 4.0)
    high = jnp.where(outer, WEIGHTS[0], WEIGHTS[1]).astype(jnp.float32) * (WEIGHTS[1] / 4.0)
    state = [given_ref[0, i] for i in range(4)]
    for i in range(4):
        out_ref[0, i] = state[i]
    for n in range(1, 16):
        for i in range(4):
            out_ref[n, i] = state[i]
        if n == 15:
            break
        part = (state[0] + state[3]) * low + (state[1] + state[2]) * high
        part = part + pltpu.roll(part, 4, 0)
        mean = part + pltpu.roll(part, 2, 0)
        state = [mean + factor * (state[i] - mean) + given_ref[n, i] for i in range(4)]


def final_kernel(slab_ref, pieces_ref, opening_ref, plain_ref, factor_ref, end_ref, sum_ref):
    later = jnp.where(slab_ref[0] == 0, 0.0, 1.0).astype(jnp.float32)
    total = jnp.zeros((8, 128), jnp.float32)
    for v in range(4):
        factor = factor_ref[v]
        starts = []
        for i in range(4):
            starts += exchange([pieces_ref[v * 4 + q, i] for q in range(4)])
        mean = weighted_mean(starts)
        squares = []
        for n in range(16):
            k = v * 16 + n
            end_ref[k] = later * (mean + factor * (starts[n] - mean)) + plain_ref[k]
            jump = later * (starts[n] - opening_ref[k])
            squares.append(jump * jump)
        total = total + weighted_mean(squares)
    total = jnp.sum(total, axis=(0, 1), keepdims=True)
    sum_ref[...] = jnp.broadcast_to(total[:, None], sum_ref.shape)


def ring(axis, shift):
    count = lax.axis_size(axis)
    return [(i, (i + shift) % count) for i in range(count)]


def on_device(slab_starts, coarse_factor, blend_weight, blend_flags):
    f32 = jnp.float32
    vmem = pl.BlockSpec(memory_space=pltpu.VMEM)
    smem = pl.BlockSpec(memory_space=pltpu.SMEM)
    opening = slab_starts.reshape(64, 8, 128)
    slab = lax.axis_index(TM).astype(jnp.int32).reshape(1)
    blend = blend_flags.astype(f32) * blend_weight
    own = jnp.concatenate([opening, blend[None]], axis=0)
    left = lax.ppermute(own, SPACE, ring(SPACE, 1))
    right = lax.ppermute(own, SPACE, ring(SPACE, -1))
    packed, plain = pl.pallas_call(
        fine_kernel,
        out_shape=(
            jax.ShapeDtypeStruct((16, 4, 8, 128), f32),
            jax.ShapeDtypeStruct((64, 8, 128), f32),
        ),
        in_specs=[smem] + [vmem] * 4,
        out_specs=[vmem] * 2,
        scratch_shapes=[
            pltpu.VMEM((64, ROWS, 128), f32),
            pltpu.VMEM((64, ROWS, 128), f32),
            pltpu.VMEM((ROWS, 128), f32),
            pltpu.VMEM((7 * 16, ROWS, 128), f32),
            pltpu.VMEM((16, ROWS, 128), f32),
        ],
        name="fine",
    )(slab, own, left, right, coarse_factor)
    gathered = lax.all_to_all(packed, TM, 0, 0)
    scanned = pl.pallas_call(
        scan_kernel,
        out_shape=jax.ShapeDtypeStruct((16, 4, 8, 128), f32),
        in_specs=[smem] + [vmem] * 2,
        out_specs=vmem,
        name="scan",
    )(slab, gathered, coarse_factor)
    starts = lax.all_to_all(scanned, TM, 0, 0)
    slab_end, partial_sums = pl.pallas_call(
        final_kernel,
        out_shape=(
            jax.ShapeDtypeStruct((64, 8, 128), f32),
            jax.ShapeDtypeStruct((16, 1, 128), f32),
        ),
        in_specs=[smem] + [vmem] * 4,
        out_specs=[vmem] * 2,
        name="final",
    )(slab, starts, opening, plain, coarse_factor)
    shared = lax.all_to_all(partial_sums, SPACE, 0, 0)
    element_count = lax.axis_size(SPACE) * slab_starts.shape[4] * slab_starts.shape[5]
    jump_norm = jnp.sqrt(jnp.sum(shared[:, 0, 0]) / element_count)
    return (slab_end.reshape(slab_starts.shape), jump_norm[None])


def solution(mesh):
    split = Mesh(mesh.devices.reshape(8, 2, 4, 4), ("tm_0", "tm_1", "space_0", "space_1"))
    return jax.shard_map(
        on_device,
        mesh=split,
        in_specs=(
            P(TM, None, None, None, SPACE, None),
            P(None, SPACE, None),
            P(SPACE, None),
            P(SPACE, None),
        ),
        out_specs=(P(TM, None, None, None, SPACE, None), P(TM)),
        check_vma=False,
    )
```

```python
import math

import jax
import jax.numpy as jnp
import numpy as np
from jax import lax
from jax.experimental import pallas as pl
from jax.experimental.pallas import tpu as pltpu
from jax.sharding import Mesh
from jax.sharding import PartitionSpec as P

FSTEPS = 4
SPACE = ("space_0", "space_1")
TM = ("tm_0", "tm_1")
STEP = 0.003
WEIGHTS = (1.0 / 6.0, 5.0 / 6.0, 5.0 / 6.0, 1.0 / 6.0)
ROWS = 32


def derivative_table():
    inner = 1.0 / math.sqrt(5.0)
    points = np.array([-1.0, -inner, inner, 1.0])
    scales = np.array(
        [1.0 / np.prod([points[c] - points[o] for o in range(4) if o != c]) for c in range(4)]
    )
    table = np.zeros((4, 4))
    for r in range(4):
        for c in range(4):
            if r != c:
                table[r, c] = scales[c] / scales[r] / (points[r] - points[c])
        table[r, r] = -np.sum(table[r])
    return table


SPLIT = [[float(2.0 * WEIGHTS[i] * derivative_table()[i, k]) for k in range(4)] for i in range(4)]
EDGE = SPLIT[0][1]
SERIES = (105.0 / 52.5, 35.0 / 52.5, 21.0 / 52.5, 15.0 / 52.5)
BINARY = tuple(x / math.log(2.0) for x in SERIES)
BETA = 0.2 / math.log(2.0)
SOUND = math.sqrt(1.4 * BETA)


def log_parts(left, right, log_left, log_right, terms):
    total = left + right
    differ = right - left
    ratio = differ / total
    ratio = ratio * ratio
    nearly = ratio < 0.0001
    series = terms[0] + ratio * (terms[1] + ratio * (terms[2] + ratio * terms[3]))
    return jnp.where(nearly, total, differ), jnp.where(nearly, series, log_right - log_left)


def pair_flux(a, b, scale=None):
    top, bottom = log_parts(a["rho"], b["rho"], a["lrho"], b["lrho"], SERIES)
    mean = top / bottom
    top, bottom = log_parts(a["beta"], b["beta"], a["lbeta"], b["lbeta"], BINARY)
    thermal = bottom / top
    normal = a["n"] + b["n"]
    pressure = a["p"] + b["p"]
    cross = a["p"] * b["n"] + b["p"] * a["n"]
    if scale is not None:
        mean = mean * scale
        pressure = pressure * scale
        cross = cross * scale
    mass = mean * normal
    half = 0.5 * mass
    kinetic = a["n"] * b["n"] + a["t"] * b["t"] + thermal
    return (
        mass,
        half * normal + pressure,
        half * (a["t"] + b["t"]),
        half * kinetic + cross,
    )


def conserved(node):
    return (node["rho"], node["mn"], node["mt"], node["e"])


def face_flux(a, b, scale):
    central = pair_flux(a, b)
    speed = jnp.maximum(jnp.abs(a["n"]) + a["c"], jnp.abs(b["n"]) + b["c"])
    return tuple(
        scale * (c - speed * (ub - ua)) for c, ua, ub in zip(central, conserved(a), conserved(b), strict=True)
    )


def physical(node):
    return (
        node["mn"],
        node["mn"] * node["n"] + node["p"],
        node["mt"] * node["n"],
        node["n"] * (node["e"] + node["p"]),
    )


def line_walls(nodes, split_share, sub_share):
    pair = {}
    for i in range(4):
        for k in range(i + 1, 4):
            scale = None if k - i == 1 and i != 1 else SPLIT[i][k] / EDGE
            pair[i, k] = pair_flux(nodes[i], nodes[k], scale)
    own = [physical(node) for node in nodes]
    speeds = [jnp.abs(node["n"]) + node["c"] for node in nodes]
    out = [[], [], []]
    for v in range(4):
        far = pair[0, 3][v]
        left, right = far + pair[0, 2][v], far + pair[1, 3][v]
        walls = (
            left + pair[0, 1][v],
            (left + pair[1, 3][v]) + pair[1, 2][v],
            right + pair[2, 3][v],
        )
        for m in range(3):
            speed = jnp.maximum(speeds[m], speeds[m + 1])
            jump = conserved(nodes[m + 1])[v] - conserved(nodes[m])[v]
            sub = own[m][v] + own[m + 1][v] - speed * jump
            out[m].append(split_share * walls[m] + sub_share * sub)
    return out


ORDER = {1: (0, 1, 2, 3), 2: (0, 2, 1, 3)}
VX, VY, PR, LR, BE, LB, CS = range(7)


def at(v, i, j):
    return v * 16 + i * 4 + j


def fine_kernel(
    slab_ref, own_ref, left_ref, right_ref, factor_ref, packed_ref, plain_ref,
    base, mid, blend_ref, prim, faces,
):
    def copy_in(k, carry):
        base[k, 0:8, :] = left_ref[k]
        base[k, 8:16, :] = own_ref[k]
        base[k, 16:24, :] = right_ref[k]
        return carry

    lax.fori_loop(0, 64, copy_in, 0, unroll=8)
    blend_ref[0:8, :] = left_ref[64] * left_ref[65]
    blend_ref[8:16, :] = own_ref[64] * own_ref[65]
    blend_ref[16:24, :] = right_ref[64] * right_ref[65]
    blend_ref[24:32, :] = jnp.zeros((8, 128), jnp.float32)

    def rows(c, offset):
        return pl.ds(pl.multiple_of(c * 8, 8) + offset, 8)

    def node_pass(src, c):
        here = rows(c, 0)
        for n in range(16):
            rho = src[n, here, :]
            inv = 1.0 / rho
            mx = src[16 + n, here, :]
            my = src[32 + n, here, :]
            vx = mx * inv
            vy = my * inv
            p = 0.4 * src[48 + n, here, :] - 0.2 * (mx * vx + my * vy)
            beta = BETA * rho / p
            prim[VX * 16 + n, here, :] = vx
            prim[VY * 16 + n, here, :] = vy
            prim[PR * 16 + n, here, :] = p
            prim[LR * 16 + n, here, :] = jnp.log(rho)
            prim[BE * 16 + n, here, :] = beta
            prim[LB * 16 + n, here, :] = jnp.log2(beta)
            prim[CS * 16 + n, here, :] = SOUND * lax.rsqrt(beta)

    def node(src, i, j, here, axis):
        n = i * 4 + j
        normal, along = (VX, VY) if axis == 1 else (VY, VX)
        order = ORDER[axis]
        return {
            "rho": src[n, here, :],
            "mn": src[order[1] * 16 + n, here, :],
            "mt": src[order[2] * 16 + n, here, :],
            "e": src[48 + n, here, :],
            "n": prim[normal * 16 + n, here, :],
            "t": prim[along * 16 + n, here, :],
            "p": prim[PR * 16 + n, here, :],
            "lrho": prim[LR * 16 + n, here, :],
            "beta": prim[BE * 16 + n, here, :],
            "lbeta": prim[LB * 16 + n, here, :],
            "c": prim[CS * 16 + n, here, :],
        }

    def face_pass(src, c, scale):
        for j in range(4):
            flux = face_flux(node(src, 3, j, rows(c, 0), 1), node(src, 0, j, rows(c, 1), 1), scale)
            for v in range(4):
                faces[j * 4 + v, rows(c, 0), :] = flux[v]

    def update_pass(src, dst, c, second):
        here = rows(c, 1)
        blend = blend_ref[rows(c, 0), :]
        scale = (0.5 if second else 1.0) * STEP / WEIGHTS[1]
        sub_share = scale * blend
        split_share = (scale - sub_share) * EDGE
        for j in range(4):
            walls = line_walls(
                [node(src, i, j, here, 1) for i in range(4)], split_share, sub_share
            )
            for v in range(4):
                column = [faces[j * 4 + v, rows(c, 0), :]]
                column += [walls[m][v] for m in range(3)]
                column += [faces[j * 4 + v, here, :]]
                for i in range(4):
                    k = at(v, i, j)
                    change = column[i + 1] - column[i]
                    if i in (0, 3):
                        change = (WEIGHTS[1] / WEIGHTS[0]) * change
                    if second:
                        start = 0.5 * (dst[k, rows(c, 2), :] + src[k, here, :])
                    else:
                        start = src[k, here, :]
                    dst[k, rows(c, 0), :] = start - change
        for i in range(4):
            nodes = [node(src, i, j, here, 2) for j in range(4)]
            behind = {key: pltpu.roll(x, 1, 1) for key, x in nodes[3].items()}
            low = face_flux(behind, nodes[0], scale)
            high = tuple(pltpu.roll(x, 127, 1) for x in low)
            walls = line_walls(nodes, split_share, sub_share)
            for q in range(4):
                v = ORDER[2][q]
                column = [low[q]] + [walls[m][q] for m in range(3)] + [high[q]]
                for j in range(4):
                    k = at(v, i, j)
                    change = column[j + 1] - column[j]
                    if j in (0, 3):
                        change = (WEIGHTS[1] / WEIGHTS[0]) * change
                    dst[k, rows(c, 0), :] = dst[k, rows(c, 0), :] - change

    def stage(src, dst, s, second):
        for c in range(3):
            blend_ref[8 * c : 8 * c + 8, :] = blend_ref[8 * c + 1 : 8 * c + 9, :]

        def run(body, count):
            def step(c, carry):
                body(c)
                return carry

            lax.fori_loop(0, lax.shift_right_logical(count - 2 * s, 3), step, 0)

        run(lambda c: node_pass(src, c), 31)
        scale = (0.5 if second else 1.0) * STEP / WEIGHTS[1]
        run(lambda c: face_pass(src, c, scale), 30)
        run(lambda c: update_pass(src, dst, c, second), 29)

    def time_step(t, carry):
        stage(base, mid, 2 * t, False)
        stage(mid, base, 2 * t + 1, True)
        return carry

    lax.fori_loop(0, FSTEPS, time_step, 0)

    later = jnp.where(slab_ref[0] == 0, 0.0, 1.0).astype(jnp.float32)
    for v in range(4):
        factor = factor_ref[v]
        mean = weighted_mean([own_ref[v * 16 + n] for n in range(16)])
        for i in range(4):
            kept = []
            for j in range(4):
                k = at(v, i, j)
                guess = mean + factor * (own_ref[k] - mean)
                kept.append(base[k, 0:8, :] - later * guess)
                plain_ref[k] = kept[j]
            for q, piece in enumerate(exchange(kept)):
                packed_ref[v * 4 + q, i] = piece


def weighted_mean(values):
    total = None
    for n, x in enumerate(values):
        term = (WEIGHTS[n // 4] * WEIGHTS[n % 4] / 4.0) * x
        total = term if total is None else total + term
    return total


def exchange(blocks):
    group = lax.broadcasted_iota(jnp.int32, (8, 128), 0) // 2
    out = []
    for q in range(4):
        piece = None
        for j in range(4):
            shift = (2 * (j - q)) % 8
            moved = pltpu.roll(blocks[j], shift, 0) if shift else blocks[j]
            piece = moved if piece is None else jnp.where(group == j, moved, piece)
        out.append(piece)
    return out


def scan_kernel(slab_ref, given_ref, factor_ref, out_ref):
    slab = slab_ref[0]
    var = lax.shift_right_logical(slab, 2)
    first = 2 * (slab & 3)
    row = lax.broadcasted_iota(jnp.int32, (8, 128), 0)
    even = jnp.broadcast_to(factor_ref[var, pl.ds(first, 1), :], (8, 128))
    odd = jnp.broadcast_to(factor_ref[var, pl.ds(first + 1, 1), :], (8, 128))
    factor = jnp.where((row & 1) == 0, even, odd)
    outer = (row < 2) | (row >= 6)
    low = jnp.where(outer, WEIGHTS[0], WEIGHTS[1]).astype(jnp.float32) * (WEIGHTS[0] / 4.0)
    high = jnp.where(outer, WEIGHTS[0], WEIGHTS[1]).astype(jnp.float32) * (WEIGHTS[1] / 4.0)
    state = [given_ref[0, i] for i in range(4)]
    for i in range(4):
        out_ref[0, i] = state[i]
    for n in range(1, 16):
        for i in range(4):
            out_ref[n, i] = state[i]
        if n == 15:
            break
        part = (state[0] + state[3]) * low + (state[1] + state[2]) * high
        part = part + pltpu.roll(part, 4, 0)
        mean = part + pltpu.roll(part, 2, 0)
        state = [mean + factor * (state[i] - mean) + given_ref[n, i] for i in range(4)]


def final_kernel(slab_ref, pieces_ref, opening_ref, plain_ref, factor_ref, end_ref, sum_ref):
    later = jnp.where(slab_ref[0] == 0, 0.0, 1.0).astype(jnp.float32)
    total = jnp.zeros((8, 128), jnp.float32)
    for v in range(4):
        factor = factor_ref[v]
        starts = []
        for i in range(4):
            starts += exchange([pieces_ref[v * 4 + q, i] for q in range(4)])
        mean = weighted_mean(starts)
        squares = []
        for n in range(16):
            k = v * 16 + n
            end_ref[k] = later * (mean + factor * (starts[n] - mean)) + plain_ref[k]
            jump = later * (starts[n] - opening_ref[k])
            squares.append(jump * jump)
        total = total + weighted_mean(squares)
    total = jnp.sum(total, axis=(0, 1), keepdims=True)
    sum_ref[...] = jnp.broadcast_to(total[:, None], sum_ref.shape)


def hold(x):
    return pltpu.with_memory_space_constraint(x, pltpu.VMEM)


def ring(axis, shift):
    count = lax.axis_size(axis)
    return [(i, (i + shift) % count) for i in range(count)]


def on_device(slab_starts, coarse_factor, blend_weight, blend_flags):
    f32 = jnp.float32
    vmem = pl.BlockSpec(memory_space=pltpu.VMEM)
    smem = pl.BlockSpec(memory_space=pltpu.SMEM)
    opening = slab_starts.reshape(64, 8, 128)
    slab = lax.axis_index(TM).astype(jnp.int32).reshape(1)
    own = jnp.concatenate([opening, blend_weight[None], blend_flags[None].astype(f32)], axis=0)
    left = lax.ppermute(own, SPACE, ring(SPACE, 1))
    right = lax.ppermute(own, SPACE, ring(SPACE, -1))
    packed, plain = pl.pallas_call(
        fine_kernel,
        out_shape=(
            pltpu.VMEM((16, 4, 8, 128), f32),
            pltpu.VMEM((64, 8, 128), f32),
        ),
        in_specs=[smem] + [vmem] * 4,
        out_specs=[vmem] * 2,
        scratch_shapes=[
            pltpu.VMEM((64, ROWS, 128), f32),
            pltpu.VMEM((64, ROWS, 128), f32),
            pltpu.VMEM((ROWS, 128), f32),
            pltpu.VMEM((7 * 16, ROWS, 128), f32),
            pltpu.VMEM((16, ROWS, 128), f32),
        ],
        name="fine",
    )(slab, hold(own), hold(left), hold(right), coarse_factor)
    gathered = lax.all_to_all(packed, TM, 0, 0)
    scanned = pl.pallas_call(
        scan_kernel,
        out_shape=pltpu.VMEM((16, 4, 8, 128), f32),
        in_specs=[smem] + [vmem] * 2,
        out_specs=vmem,
        name="scan",
    )(slab, hold(gathered), coarse_factor)
    starts = lax.all_to_all(scanned, TM, 0, 0)
    slab_end, partial_sums = pl.pallas_call(
        final_kernel,
        out_shape=(
            jax.ShapeDtypeStruct((64, 8, 128), f32),
            pltpu.VMEM((16, 1, 128), f32),
        ),
        in_specs=[smem] + [vmem] * 4,
        out_specs=[vmem] * 2,
        name="final",
    )(slab, hold(starts), opening, hold(plain), coarse_factor)
    shared = lax.all_to_all(partial_sums, SPACE, 0, 0)
    element_count = lax.axis_size(SPACE) * slab_starts.shape[4] * slab_starts.shape[5]
    jump_norm = jnp.sqrt(jnp.sum(shared[:, 0, 0]) / element_count)
    return (slab_end.reshape(slab_starts.shape), jump_norm[None])


def solution(mesh):
    split = Mesh(mesh.devices.reshape(8, 2, 4, 4), ("tm_0", "tm_1", "space_0", "space_1"))
    return jax.shard_map(
        on_device,
        mesh=split,
        in_specs=(
            P(TM, None, None, None, SPACE, None),
            P(None, SPACE, None),
            P(SPACE, None),
            P(SPACE, None),
        ),
        out_specs=(P(TM, None, None, None, SPACE, None), P(TM)),
        check_vma=False,
    )
```

```python
import math

import jax
import jax.numpy as jnp
import numpy as np
from jax import lax
from jax.experimental import pallas as pl
from jax.experimental.pallas import tpu as pltpu
from jax.sharding import Mesh
from jax.sharding import PartitionSpec as P

FSTEPS = 4
SPACE = ("space_0", "space_1")
TM = ("tm_0", "tm_1")
STEP = 0.003
WEIGHTS = (1.0 / 6.0, 5.0 / 6.0, 5.0 / 6.0, 1.0 / 6.0)


def derivative_table():
    inner = 1.0 / math.sqrt(5.0)
    points = np.array([-1.0, -inner, inner, 1.0])
    scales = np.array(
        [1.0 / np.prod([points[c] - points[o] for o in range(4) if o != c]) for c in range(4)]
    )
    table = np.zeros((4, 4))
    for r in range(4):
        for c in range(4):
            if r != c:
                table[r, c] = scales[c] / scales[r] / (points[r] - points[c])
        table[r, r] = -np.sum(table[r])
    return table


SPLIT = [[float(2.0 * WEIGHTS[i] * derivative_table()[i, k]) for k in range(4)] for i in range(4)]
EDGE = SPLIT[0][1]
SERIES = (105.0 / 52.5, 35.0 / 52.5, 21.0 / 52.5, 15.0 / 52.5)
BINARY = tuple(x / math.log(2.0) for x in SERIES)
BETA = 0.2 / math.log(2.0)
SOUND = math.sqrt(1.4 * BETA)


def log_parts(left, right, log_left, log_right, terms):
    total = left + right
    differ = right - left
    ratio = differ / total
    ratio = ratio * ratio
    nearly = ratio < 0.0001
    series = terms[0] + ratio * (terms[1] + ratio * (terms[2] + ratio * terms[3]))
    return jnp.where(nearly, total, differ), jnp.where(nearly, series, log_right - log_left)


def pair_flux(a, b, scale=None):
    top, bottom = log_parts(a["rho"], b["rho"], a["lrho"], b["lrho"], SERIES)
    mean = top / bottom
    top, bottom = log_parts(a["beta"], b["beta"], a["lbeta"], b["lbeta"], BINARY)
    thermal = bottom / top
    normal = a["n"] + b["n"]
    pressure = a["p"] + b["p"]
    cross = a["p"] * b["n"] + b["p"] * a["n"]
    if scale is not None:
        mean = mean * scale
        pressure = pressure * scale
        cross = cross * scale
    mass = mean * normal
    half = 0.5 * mass
    kinetic = a["n"] * b["n"] + a["t"] * b["t"] + thermal
    return (
        mass,
        half * normal + pressure,
        half * (a["t"] + b["t"]),
        half * kinetic + cross,
    )


def conserved(node):
    return (node["rho"], node["mn"], node["mt"], node["e"])


def face_flux(a, b, scale):
    central = pair_flux(a, b)
    speed = jnp.maximum(jnp.abs(a["n"]) + a["c"], jnp.abs(b["n"]) + b["c"])
    return tuple(
        scale * (c - speed * (ub - ua)) for c, ua, ub in zip(central, conserved(a), conserved(b), strict=True)
    )


def physical(node):
    return (
        node["mn"],
        node["mn"] * node["n"] + node["p"],
        node["mt"] * node["n"],
        node["n"] * (node["e"] + node["p"]),
    )


def line_walls(nodes, split_share, sub_share):
    pair = {}
    for i in range(4):
        for k in range(i + 1, 4):
            scale = None if k - i == 1 and i != 1 else SPLIT[i][k] / EDGE
            pair[i, k] = pair_flux(nodes[i], nodes[k], scale)
    own = [physical(node) for node in nodes]
    speeds = [jnp.abs(node["n"]) + node["c"] for node in nodes]
    out = [[], [], []]
    for v in range(4):
        far = pair[0, 3][v]
        left, right = far + pair[0, 2][v], far + pair[1, 3][v]
        walls = (
            left + pair[0, 1][v],
            (left + pair[1, 3][v]) + pair[1, 2][v],
            right + pair[2, 3][v],
        )
        for m in range(3):
            speed = jnp.maximum(speeds[m], speeds[m + 1])
            jump = conserved(nodes[m + 1])[v] - conserved(nodes[m])[v]
            sub = own[m][v] + own[m + 1][v] - speed * jump
            out[m].append(split_share * walls[m] + sub_share * sub)
    return out


ORDER = {1: (0, 1, 2, 3), 2: (0, 2, 1, 3)}
VX, VY, PR, LR, BE, LB, CS = range(7)


def at(v, i, j):
    return v * 16 + i * 4 + j


def rows(c, offset):
    start = c * 8 + offset
    if isinstance(c, int):
        return pl.ds(start, 8)
    return pl.ds(pl.multiple_of(c * 8, 8) + offset, 8)


def node_pass(src, prim, c):
    here = rows(c, 0)
    for n in range(16):
        rho = src[n, here, :]
        inv = 1.0 / rho
        mx = src[16 + n, here, :]
        my = src[32 + n, here, :]
        vx = mx * inv
        vy = my * inv
        p = 0.4 * src[48 + n, here, :] - 0.2 * (mx * vx + my * vy)
        beta = BETA * rho / p
        prim[VX * 16 + n, here, :] = vx
        prim[VY * 16 + n, here, :] = vy
        prim[PR * 16 + n, here, :] = p
        prim[LR * 16 + n, here, :] = jnp.log(rho)
        prim[BE * 16 + n, here, :] = beta
        prim[LB * 16 + n, here, :] = jnp.log2(beta)
        prim[CS * 16 + n, here, :] = SOUND * lax.rsqrt(beta)


def node(src, prim, i, j, here, axis):
    n = i * 4 + j
    normal, along = (VX, VY) if axis == 1 else (VY, VX)
    order = ORDER[axis]
    return {
        "rho": src[n, here, :],
        "mn": src[order[1] * 16 + n, here, :],
        "mt": src[order[2] * 16 + n, here, :],
        "e": src[48 + n, here, :],
        "n": prim[normal * 16 + n, here, :],
        "t": prim[along * 16 + n, here, :],
        "p": prim[PR * 16 + n, here, :],
        "lrho": prim[LR * 16 + n, here, :],
        "beta": prim[BE * 16 + n, here, :],
        "lbeta": prim[LB * 16 + n, here, :],
        "c": prim[CS * 16 + n, here, :],
    }


def face_pass(src, prim, faces, c, scale):
    for j in range(4):
        lower = node(src, prim, 3, j, rows(c, 0), 1)
        flux = face_flux(lower, node(src, prim, 0, j, rows(c, 1), 1), scale)
        for v in range(4):
            faces[j * 4 + v, rows(c, 0), :] = flux[v]


def update_pass(src, dst, prim, faces, c, blend, second, right):
    here = rows(c, 1)
    there, start_rows = (rows(c, 2), rows(c, 0)) if right else (rows(c, 0), rows(c, 2))
    scale = (0.5 if second else 1.0) * STEP / WEIGHTS[1]
    sub_share = scale * blend
    split_share = (scale - sub_share) * EDGE
    for j in range(4):
        nodes = [node(src, prim, i, j, here, 1) for i in range(4)]
        walls = line_walls(nodes, split_share, sub_share)
        for v in range(4):
            column = [faces[j * 4 + v, rows(c, 0), :]]
            column += [walls[m][v] for m in range(3)]
            column += [faces[j * 4 + v, here, :]]
            for i in range(4):
                k = at(v, i, j)
                change = column[i + 1] - column[i]
                if i in (0, 3):
                    change = (WEIGHTS[1] / WEIGHTS[0]) * change
                if second:
                    start = 0.5 * (dst[k, start_rows, :] + src[k, here, :])
                else:
                    start = src[k, here, :]
                dst[k, there, :] = start - change
    for i in range(4):
        nodes = [node(src, prim, i, j, here, 2) for j in range(4)]
        behind = {key: pltpu.roll(x, 1, 1) for key, x in nodes[3].items()}
        low = face_flux(behind, nodes[0], scale)
        high = tuple(pltpu.roll(x, 127, 1) for x in low)
        walls = line_walls(nodes, split_share, sub_share)
        for q in range(4):
            v = ORDER[2][q]
            column = [low[q]] + [walls[m][q] for m in range(3)] + [high[q]]
            for j in range(4):
                k = at(v, i, j)
                change = column[j + 1] - column[j]
                if j in (0, 3):
                    change = (WEIGHTS[1] / WEIGHTS[0]) * change
                dst[k, there, :] = dst[k, there, :] - change


def loop(count, body):
    if isinstance(count, int) and count == 1:
        body(0)
        return

    def step(c, carry):
        body(c)
        return carry

    lax.fori_loop(0, count, step, 0)


def stage(src, dst, work, second, right, chunks, blend_at, updates):
    prim, faces = work
    scale = (0.5 if second else 1.0) * STEP / WEIGHTS[1]
    loop(chunks, lambda c: node_pass(src, prim, c))
    loop(chunks, lambda c: face_pass(src, prim, faces, c, scale))
    loop(
        updates, lambda c: update_pass(src, dst, prim, faces, c, blend_at(c), second, right)
    )


def inner_kernel(own_ref, inner_ref, base, mid, prim, faces):
    for k in range(64):
        base[k, 0:8, :] = own_ref[k]
    blend = own_ref[64] * own_ref[65]
    for s in range(1, 4):
        second = s == 2
        src, dst = (mid, base) if second else (base, mid)
        shifted = pltpu.roll(blend, 8 - s, 0)
        stage(src, dst, (prim, faces), second, False, 1, lambda c: shifted, 1)
        for k in range(64):
            inner_ref[s - 1, k] = dst[k, 0:8, :]


def right_kernel(own_ref, right_ref, inner_ref, out_ref, base, mid, prim, faces, blend_ref):
    for k in range(64):
        base[k, 0:2, :] = own_ref[k, 6:8, :]
        base[k, 2:10, :] = right_ref[k]
    blend_ref[0:8, :] = own_ref[64] * own_ref[65]
    blend_ref[8:16, :] = right_ref[64] * right_ref[65]

    def fill(dst, s):
        def one(k, carry):
            dst[k, 0:2, :] = inner_ref[s - 1, k, pl.ds(6 - 2 * s, 2), :]
            return carry

        lax.fori_loop(0, 64, one, 0, unroll=16)

    def time_step(t, carry):
        for second in (False, True):
            s = 2 * t + (2 if second else 1)
            src, dst = (mid, base) if second else (base, mid)
            blend_at = lambda c, s=s: blend_ref[pl.ds(8 - s, 8), :]
            stage(src, dst, (prim, faces), second, True, 2, blend_at, 1)
            fill(dst, jnp.minimum(s, 3))
        return carry

    lax.fori_loop(0, 2, time_step, 0)
    for k in range(64):
        out_ref[k] = base[k, 2:10, :]


def fine_kernel(
    slab_ref, own_ref, left_ref, right_ref, inner_ref, strip_ref, factor_ref,
    packed_ref, plain_ref, base, mid, prim, faces, blend_ref,
):
    for k in range(64):
        base[k, 0:8, :] = left_ref[k]
        base[k, 8:10, :] = own_ref[k, 0:2, :]
    blend_ref[0:8, :] = left_ref[64] * left_ref[65]
    blend_ref[8:16, :] = own_ref[64] * own_ref[65]
    blend_ref[16:24, :] = right_ref[64] * right_ref[65]

    def fill(dst, s):
        @pl.when(s < 4)
        def _():
            def one(k, carry):
                dst[k, 8:10, :] = inner_ref[s - 1, k, 0:2, :]
                return carry

            lax.fori_loop(0, 64, one, 0, unroll=16)

        @pl.when(s == 4)
        def _():
            def one(k, carry):
                dst[k, 8:16, :] = strip_ref[k]
                return carry

            lax.fori_loop(0, 64, one, 0, unroll=16)

    def time_step(t, carry):
        for second in (False, True):
            s = 2 * t + (2 if second else 1)
            src, dst = (mid, base) if second else (base, mid)
            blend_at = lambda c, s=s: blend_ref[pl.ds(8 * c + s, 8), :]
            updates = jnp.where((s > 4) & (s < 8), 2, 1)
            stage(src, dst, (prim, faces), second, False, 2, blend_at, updates)
            fill(dst, s)
        return carry

    lax.fori_loop(0, FSTEPS, time_step, 0)

    later = jnp.where(slab_ref[0] == 0, 0.0, 1.0).astype(jnp.float32)
    for v in range(4):
        factor = factor_ref[v]
        mean = weighted_mean([own_ref[v * 16 + n, :, :] for n in range(16)])
        for i in range(4):
            kept = []
            for j in range(4):
                k = at(v, i, j)
                guess = mean + factor * (own_ref[k] - mean)
                kept.append(base[k, 0:8, :] - later * guess)
                plain_ref[k] = kept[j]
            for q, piece in enumerate(exchange(kept)):
                packed_ref[v * 4 + q, i] = piece


def weighted_mean(values):
    total = None
    for n, x in enumerate(values):
        term = (WEIGHTS[n // 4] * WEIGHTS[n % 4] / 4.0) * x
        total = term if total is None else total + term
    return total


def exchange(blocks):
    group = lax.broadcasted_iota(jnp.int32, (8, 128), 0) // 2
    out = []
    for q in range(4):
        piece = None
        for j in range(4):
            shift = (2 * (j - q)) % 8
            moved = pltpu.roll(blocks[j], shift, 0) if shift else blocks[j]
            piece = moved if piece is None else jnp.where(group == j, moved, piece)
        out.append(piece)
    return out


def scan_kernel(slab_ref, given_ref, factor_ref, out_ref):
    slab = slab_ref[0]
    var = lax.shift_right_logical(slab, 2)
    first = 2 * (slab & 3)
    row = lax.broadcasted_iota(jnp.int32, (8, 128), 0)
    even = jnp.broadcast_to(factor_ref[var, pl.ds(first, 1), :], (8, 128))
    odd = jnp.broadcast_to(factor_ref[var, pl.ds(first + 1, 1), :], (8, 128))
    factor = jnp.where((row & 1) == 0, even, odd)
    outer = (row < 2) | (row >= 6)
    low = jnp.where(outer, WEIGHTS[0], WEIGHTS[1]).astype(jnp.float32) * (WEIGHTS[0] / 4.0)
    high = jnp.where(outer, WEIGHTS[0], WEIGHTS[1]).astype(jnp.float32) * (WEIGHTS[1] / 4.0)
    state = [given_ref[0, i] for i in range(4)]
    for i in range(4):
        out_ref[0, i] = state[i]
    for n in range(1, 16):
        for i in range(4):
            out_ref[n, i] = state[i]
        if n == 15:
            break
        part = (state[0] + state[3]) * low + (state[1] + state[2]) * high
        part = part + pltpu.roll(part, 4, 0)
        mean = part + pltpu.roll(part, 2, 0)
        state = [mean + factor * (state[i] - mean) + given_ref[n, i] for i in range(4)]


def final_kernel(slab_ref, pieces_ref, opening_ref, plain_ref, factor_ref, end_ref, sum_ref):
    later = jnp.where(slab_ref[0] == 0, 0.0, 1.0).astype(jnp.float32)
    total = jnp.zeros((8, 128), jnp.float32)
    for v in range(4):
        factor = factor_ref[v]
        starts = []
        for i in range(4):
            starts += exchange([pieces_ref[v * 4 + q, i] for q in range(4)])
        mean = weighted_mean(starts)
        squares = []
        for n in range(16):
            k = v * 16 + n
            end_ref[k] = later * (mean + factor * (starts[n] - mean)) + plain_ref[k]
            jump = later * (starts[n] - opening_ref[k])
            squares.append(jump * jump)
        total = total + weighted_mean(squares)
    total = jnp.sum(total, axis=(0, 1), keepdims=True)
    sum_ref[...] = jnp.broadcast_to(total[:, None], sum_ref.shape)


def hold(x):
    return pltpu.with_memory_space_constraint(x, pltpu.VMEM)


def work(count):
    shapes = [(64, count, 128), (64, count, 128), (7 * 16, count, 128), (16, count, 128)]
    return [pltpu.VMEM(shape, jnp.float32) for shape in shapes]


def estimate(updates):
    return pl.CostEstimate(
        flops=updates * 400_000_000, transcendentals=0, bytes_accessed=updates * 1_000_000
    )


def ring(axis, shift):
    count = lax.axis_size(axis)
    return [(i, (i + shift) % count) for i in range(count)]


def on_device(slab_starts, coarse_factor, blend_weight, blend_flags):
    f32 = jnp.float32
    vmem = pl.BlockSpec(memory_space=pltpu.VMEM)
    smem = pl.BlockSpec(memory_space=pltpu.SMEM)
    opening = slab_starts.reshape(64, 8, 128)
    slab = lax.axis_index(TM).astype(jnp.int32).reshape(1)
    own = jnp.concatenate([opening, blend_weight[None], blend_flags[None].astype(f32)], axis=0)
    left = lax.ppermute(own, SPACE, ring(SPACE, 1))
    right = lax.ppermute(own, SPACE, ring(SPACE, -1))
    own, left, right = hold(own), hold(left), hold(right)
    inner = pl.pallas_call(
        inner_kernel,
        out_shape=pltpu.VMEM((3, 64, 8, 128), f32),
        in_specs=[vmem],
        out_specs=vmem,
        scratch_shapes=work(16),
        cost_estimate=estimate(3),
        name="inner",
    )(own)
    strip = pl.pallas_call(
        right_kernel,
        out_shape=pltpu.VMEM((64, 8, 128), f32),
        in_specs=[vmem] * 3,
        out_specs=vmem,
        scratch_shapes=work(24) + [pltpu.VMEM((24, 128), f32)],
        cost_estimate=estimate(4),
        name="right",
    )(own, right, hold(inner))
    packed, plain = pl.pallas_call(
        fine_kernel,
        out_shape=(
            pltpu.VMEM((16, 4, 8, 128), f32),
            pltpu.VMEM((64, 8, 128), f32),
        ),
        in_specs=[smem] + [vmem] * 6,
        out_specs=[vmem] * 2,
        scratch_shapes=work(24) + [pltpu.VMEM((24, 128), f32)],
        cost_estimate=estimate(11),
        name="fine",
    )(slab, own, left, right, hold(inner), hold(strip), coarse_factor)
    gathered = lax.all_to_all(packed, TM, 0, 0)
    scanned = pl.pallas_call(
        scan_kernel,
        out_shape=pltpu.VMEM((16, 4, 8, 128), f32),
        in_specs=[smem] + [vmem] * 2,
        out_specs=vmem,
        name="scan",
    )(slab, hold(gathered), coarse_factor)
    starts = lax.all_to_all(scanned, TM, 0, 0)
    slab_end, partial_sums = pl.pallas_call(
        final_kernel,
        out_shape=(
            jax.ShapeDtypeStruct((64, 8, 128), f32),
            pltpu.VMEM((16, 1, 128), f32),
        ),
        in_specs=[smem] + [vmem] * 4,
        out_specs=[vmem] * 2,
        name="final",
    )(slab, hold(starts), opening, hold(plain), coarse_factor)
    shared = lax.all_to_all(partial_sums, SPACE, 0, 0)
    element_count = lax.axis_size(SPACE) * slab_starts.shape[4] * slab_starts.shape[5]
    jump_norm = jnp.sqrt(jnp.sum(shared[:, 0, 0]) / element_count)
    return (slab_end.reshape(slab_starts.shape), jump_norm[None])


def solution(mesh):
    split = Mesh(mesh.devices.reshape(8, 2, 4, 4), ("tm_0", "tm_1", "space_0", "space_1"))
    return jax.shard_map(
        on_device,
        mesh=split,
        in_specs=(
            P(TM, None, None, None, SPACE, None),
            P(None, SPACE, None),
            P(SPACE, None),
            P(SPACE, None),
        ),
        out_specs=(P(TM, None, None, None, SPACE, None), P(TM)),
        check_vma=False,
    )
```

```python
import math

import jax
import jax.numpy as jnp
import numpy as np
from jax import lax
from jax.experimental import pallas as pl
from jax.experimental.pallas import tpu as pltpu
from jax.sharding import Mesh
from jax.sharding import PartitionSpec as P

FSTEPS = 4
SPACE = ("space_0", "space_1")
TM = ("tm_0", "tm_1")
STEP = 0.003
WEIGHTS = (1.0 / 6.0, 5.0 / 6.0, 5.0 / 6.0, 1.0 / 6.0)


def derivative_table():
    inner = 1.0 / math.sqrt(5.0)
    points = np.array([-1.0, -inner, inner, 1.0])
    scales = np.array(
        [1.0 / np.prod([points[c] - points[o] for o in range(4) if o != c]) for c in range(4)]
    )
    table = np.zeros((4, 4))
    for r in range(4):
        for c in range(4):
            if r != c:
                table[r, c] = scales[c] / scales[r] / (points[r] - points[c])
        table[r, r] = -np.sum(table[r])
    return table


SPLIT = [[float(2.0 * WEIGHTS[i] * derivative_table()[i, k]) for k in range(4)] for i in range(4)]
EDGE = SPLIT[0][1]
SERIES = (105.0 / 52.5, 35.0 / 52.5, 21.0 / 52.5, 15.0 / 52.5)
BINARY = tuple(x / math.log(2.0) for x in SERIES)
BETA = 0.2 / math.log(2.0)
SOUND = math.sqrt(1.4 * BETA)


def log_parts(left, right, log_left, log_right, terms):
    total = left + right
    differ = right - left
    ratio = differ / total
    ratio = ratio * ratio
    nearly = ratio < 0.0001
    series = terms[0] + ratio * (terms[1] + ratio * (terms[2] + ratio * terms[3]))
    return jnp.where(nearly, total, differ), jnp.where(nearly, series, log_right - log_left)


def pair_flux(a, b, scale=None):
    top, bottom = log_parts(a["rho"], b["rho"], a["lrho"], b["lrho"], SERIES)
    mean = top / bottom
    top, bottom = log_parts(a["beta"], b["beta"], a["lbeta"], b["lbeta"], BINARY)
    thermal = bottom / top
    normal = a["n"] + b["n"]
    pressure = a["p"] + b["p"]
    cross = a["p"] * b["n"] + b["p"] * a["n"]
    if scale is not None:
        mean = mean * scale
        pressure = pressure * scale
        cross = cross * scale
    mass = mean * normal
    half = 0.5 * mass
    kinetic = a["n"] * b["n"] + a["t"] * b["t"] + thermal
    return (
        mass,
        half * normal + pressure,
        half * (a["t"] + b["t"]),
        half * kinetic + cross,
    )


def conserved(node):
    return (node["rho"], node["mn"], node["mt"], node["e"])


def face_flux(a, b, scale):
    central = pair_flux(a, b)
    speed = jnp.maximum(jnp.abs(a["n"]) + a["c"], jnp.abs(b["n"]) + b["c"])
    return tuple(
        scale * (c - speed * (ub - ua)) for c, ua, ub in zip(central, conserved(a), conserved(b), strict=True)
    )


def physical(node):
    return (
        node["mn"],
        node["mn"] * node["n"] + node["p"],
        node["mt"] * node["n"],
        node["n"] * (node["e"] + node["p"]),
    )


def line_walls(nodes, split_share, sub_share):
    pair = {}
    for i in range(4):
        for k in range(i + 1, 4):
            scale = None if k - i == 1 and i != 1 else SPLIT[i][k] / EDGE
            pair[i, k] = pair_flux(nodes[i], nodes[k], scale)
    own = [physical(node) for node in nodes]
    speeds = [jnp.abs(node["n"]) + node["c"] for node in nodes]
    out = [[], [], []]
    for v in range(4):
        far = pair[0, 3][v]
        left, right = far + pair[0, 2][v], far + pair[1, 3][v]
        walls = (
            left + pair[0, 1][v],
            (left + pair[1, 3][v]) + pair[1, 2][v],
            right + pair[2, 3][v],
        )
        for m in range(3):
            speed = jnp.maximum(speeds[m], speeds[m + 1])
            jump = conserved(nodes[m + 1])[v] - conserved(nodes[m])[v]
            sub = own[m][v] + own[m + 1][v] - speed * jump
            out[m].append(split_share * walls[m] + sub_share * sub)
    return out


ORDER = {1: (0, 1, 2, 3), 2: (0, 2, 1, 3)}
VX, VY, PR, LR, BE, LB, CS = range(7)


def at(v, i, j):
    return v * 16 + i * 4 + j


def rows(c, offset):
    start = c * 8 + offset
    if isinstance(c, int):
        return pl.ds(start, 8)
    return pl.ds(pl.multiple_of(c * 8, 8) + offset, 8)


def node_pass(src, prim, c):
    here = rows(c, 0)
    for n in range(16):
        rho = src[n, here, :]
        inv = 1.0 / rho
        mx = src[16 + n, here, :]
        my = src[32 + n, here, :]
        vx = mx * inv
        vy = my * inv
        p = 0.4 * src[48 + n, here, :] - 0.2 * (mx * vx + my * vy)
        beta = BETA * rho / p
        prim[VX * 16 + n, here, :] = vx
        prim[VY * 16 + n, here, :] = vy
        prim[PR * 16 + n, here, :] = p
        prim[LR * 16 + n, here, :] = jnp.log(rho)
        prim[BE * 16 + n, here, :] = beta
        prim[LB * 16 + n, here, :] = jnp.log2(beta)
        prim[CS * 16 + n, here, :] = SOUND * lax.rsqrt(beta)


def node(src, prim, i, j, here, axis):
    n = i * 4 + j
    normal, along = (VX, VY) if axis == 1 else (VY, VX)
    order = ORDER[axis]
    return {
        "rho": src[n, here, :],
        "mn": src[order[1] * 16 + n, here, :],
        "mt": src[order[2] * 16 + n, here, :],
        "e": src[48 + n, here, :],
        "n": prim[normal * 16 + n, here, :],
        "t": prim[along * 16 + n, here, :],
        "p": prim[PR * 16 + n, here, :],
        "lrho": prim[LR * 16 + n, here, :],
        "beta": prim[BE * 16 + n, here, :],
        "lbeta": prim[LB * 16 + n, here, :],
        "c": prim[CS * 16 + n, here, :],
    }


def face_pass(src, prim, faces, c, scale):
    for j in range(4):
        lower = node(src, prim, 3, j, rows(c, 0), 1)
        flux = face_flux(lower, node(src, prim, 0, j, rows(c, 1), 1), scale)
        for v in range(4):
            faces[j * 4 + v, rows(c, 0), :] = flux[v]


def update_pass(src, dst, prim, faces, c, blend, second, right):
    here = rows(c, 1)
    there, start_rows = (rows(c, 2), rows(c, 0)) if right else (rows(c, 0), rows(c, 2))
    scale = (0.5 if second else 1.0) * STEP / WEIGHTS[1]
    sub_share = scale * blend
    split_share = (scale - sub_share) * EDGE
    for j in range(4):
        nodes = [node(src, prim, i, j, here, 1) for i in range(4)]
        walls = line_walls(nodes, split_share, sub_share)
        for v in range(4):
            column = [faces[j * 4 + v, rows(c, 0), :]]
            column += [walls[m][v] for m in range(3)]
            column += [faces[j * 4 + v, here, :]]
            for i in range(4):
                k = at(v, i, j)
                change = column[i + 1] - column[i]
                if i in (0, 3):
                    change = (WEIGHTS[1] / WEIGHTS[0]) * change
                if second:
                    start = 0.5 * (dst[k, start_rows, :] + src[k, here, :])
                else:
                    start = src[k, here, :]
                dst[k, there, :] = start - change
    for i in range(4):
        nodes = [node(src, prim, i, j, here, 2) for j in range(4)]
        behind = {key: pltpu.roll(x, 1, 1) for key, x in nodes[3].items()}
        low = face_flux(behind, nodes[0], scale)
        high = tuple(pltpu.roll(x, 127, 1) for x in low)
        walls = line_walls(nodes, split_share, sub_share)
        for q in range(4):
            v = ORDER[2][q]
            column = [low[q]] + [walls[m][q] for m in range(3)] + [high[q]]
            for j in range(4):
                k = at(v, i, j)
                change = column[j + 1] - column[j]
                if j in (0, 3):
                    change = (WEIGHTS[1] / WEIGHTS[0]) * change
                dst[k, there, :] = dst[k, there, :] - change


def loop(count, body):
    if isinstance(count, int) and count == 1:
        body(0)
        return

    def step(c, carry):
        body(c)
        return carry

    lax.fori_loop(0, count, step, 0)


def stage(src, dst, work, second, right, chunks, blend_at, updates):
    prim, faces = work
    scale = (0.5 if second else 1.0) * STEP / WEIGHTS[1]
    loop(chunks, lambda c: node_pass(src, prim, c))
    loop(chunks, lambda c: face_pass(src, prim, faces, c, scale))
    loop(
        updates, lambda c: update_pass(src, dst, prim, faces, c, blend_at(c), second, right)
    )


def join_kernel(opening_ref, weight_ref, flags_ref, own_ref, weight, flags, sems):
    copies = [
        pltpu.make_async_copy(opening_ref, own_ref.at[pl.ds(0, 64)], sems.at[0]),
        pltpu.make_async_copy(weight_ref, weight, sems.at[1]),
        pltpu.make_async_copy(flags_ref, flags, sems.at[2]),
    ]
    for copy in copies:
        copy.start()
    copies[1].wait()
    copies[2].wait()
    own_ref[64] = flags[...].astype(jnp.float32) * weight[...]
    copies[0].wait()


def inner_kernel(own_ref, inner_ref, base, mid, prim, faces):
    for k in range(64):
        base[k, 0:8, :] = own_ref[k]
    blend = own_ref[64]
    for s in range(1, 4):
        second = s == 2
        src, dst = (mid, base) if second else (base, mid)
        shifted = pltpu.roll(blend, 8 - s, 0)
        stage(src, dst, (prim, faces), second, False, 1, lambda c: shifted, 1)
        for k in range(64):
            inner_ref[s - 1, k] = dst[k, 0:8, :]


def right_kernel(own_ref, right_ref, inner_ref, out_ref, base, mid, prim, faces, blend_ref):
    for k in range(64):
        base[k, 0:2, :] = own_ref[k, 6:8, :]
        base[k, 2:10, :] = right_ref[k]
    blend_ref[0:8, :] = own_ref[64]
    blend_ref[8:16, :] = right_ref[64]

    def fill(dst, s):
        def one(k, carry):
            dst[k, 0:2, :] = inner_ref[s - 1, k, pl.ds(6 - 2 * s, 2), :]
            return carry

        lax.fori_loop(0, 64, one, 0, unroll=16)

    def time_step(t, carry):
        for second in (False, True):
            s = 2 * t + (2 if second else 1)
            src, dst = (mid, base) if second else (base, mid)
            blend_at = lambda c, s=s: blend_ref[pl.ds(8 - s, 8), :]
            stage(src, dst, (prim, faces), second, True, 2, blend_at, 1)
            fill(dst, jnp.minimum(s, 3))
        return carry

    lax.fori_loop(0, 2, time_step, 0)
    for k in range(64):
        out_ref[k] = base[k, 2:10, :]


def fine_kernel(
    slab_ref, own_ref, left_ref, right_ref, inner_ref, strip_ref, factor_ref,
    packed_ref, plain_ref, base, mid, prim, faces, blend_ref,
):
    for k in range(64):
        base[k, 0:8, :] = left_ref[k]
        base[k, 8:10, :] = own_ref[k, 0:2, :]
    blend_ref[0:8, :] = left_ref[64]
    blend_ref[8:16, :] = own_ref[64]
    blend_ref[16:24, :] = right_ref[64]

    def fill(dst, s):
        @pl.when(s < 4)
        def _():
            def one(k, carry):
                dst[k, 8:10, :] = inner_ref[s - 1, k, 0:2, :]
                return carry

            lax.fori_loop(0, 64, one, 0, unroll=16)

        @pl.when(s == 4)
        def _():
            def one(k, carry):
                dst[k, 8:16, :] = strip_ref[k]
                return carry

            lax.fori_loop(0, 64, one, 0, unroll=16)

    def time_step(t, carry):
        for second in (False, True):
            s = 2 * t + (2 if second else 1)
            src, dst = (mid, base) if second else (base, mid)
            blend_at = lambda c, s=s: blend_ref[pl.ds(8 * c + s, 8), :]
            updates = jnp.where((s > 4) & (s < 8), 2, 1)
            stage(src, dst, (prim, faces), second, False, 2, blend_at, updates)
            fill(dst, s)
        return carry

    lax.fori_loop(0, FSTEPS, time_step, 0)

    later = jnp.where(slab_ref[0] == 0, 0.0, 1.0).astype(jnp.float32)
    for v in range(4):
        factor = factor_ref[v]
        mean = weighted_mean([own_ref[v * 16 + n, :, :] for n in range(16)])
        for i in range(4):
            kept = []
            for j in range(4):
                k = at(v, i, j)
                guess = mean + factor * (own_ref[k] - mean)
                kept.append(base[k, 0:8, :] - later * guess)
                plain_ref[k] = kept[j]
            for q, piece in enumerate(exchange(kept)):
                packed_ref[v * 4 + q, i] = piece


def weighted_mean(values):
    total = None
    for n, x in enumerate(values):
        term = (WEIGHTS[n // 4] * WEIGHTS[n % 4] / 4.0) * x
        total = term if total is None else total + term
    return total


def exchange(blocks):
    group = lax.broadcasted_iota(jnp.int32, (8, 128), 0) // 2
    out = []
    for q in range(4):
        piece = None
        for j in range(4):
            shift = (2 * (j - q)) % 8
            moved = pltpu.roll(blocks[j], shift, 0) if shift else blocks[j]
            piece = moved if piece is None else jnp.where(group == j, moved, piece)
        out.append(piece)
    return out


def scan_kernel(slab_ref, given_ref, factor_ref, out_ref):
    slab = slab_ref[0]
    var = lax.shift_right_logical(slab, 2)
    first = 2 * (slab & 3)
    row = lax.broadcasted_iota(jnp.int32, (8, 128), 0)
    even = jnp.broadcast_to(factor_ref[var, pl.ds(first, 1), :], (8, 128))
    odd = jnp.broadcast_to(factor_ref[var, pl.ds(first + 1, 1), :], (8, 128))
    factor = jnp.where((row & 1) == 0, even, odd)
    outer = (row < 2) | (row >= 6)
    low = jnp.where(outer, WEIGHTS[0], WEIGHTS[1]).astype(jnp.float32) * (WEIGHTS[0] / 4.0)
    high = jnp.where(outer, WEIGHTS[0], WEIGHTS[1]).astype(jnp.float32) * (WEIGHTS[1] / 4.0)
    state = [given_ref[0, i] for i in range(4)]
    for i in range(4):
        out_ref[0, i] = state[i]
    for n in range(1, 16):
        for i in range(4):
            out_ref[n, i] = state[i]
        if n == 15:
            break
        part = (state[0] + state[3]) * low + (state[1] + state[2]) * high
        part = part + pltpu.roll(part, 4, 0)
        mean = part + pltpu.roll(part, 2, 0)
        state = [mean + factor * (state[i] - mean) + given_ref[n, i] for i in range(4)]


def final_kernel(slab_ref, pieces_ref, opening_ref, plain_ref, factor_ref, end_ref, sum_ref):
    later = jnp.where(slab_ref[0] == 0, 0.0, 1.0).astype(jnp.float32)
    total = jnp.zeros((8, 128), jnp.float32)
    for v in range(4):
        factor = factor_ref[v]
        starts = []
        for i in range(4):
            starts += exchange([pieces_ref[v * 4 + q, i] for q in range(4)])
        mean = weighted_mean(starts)
        squares = []
        for n in range(16):
            k = v * 16 + n
            end_ref[k] = later * (mean + factor * (starts[n] - mean)) + plain_ref[k]
            jump = later * (starts[n] - opening_ref[k])
            squares.append(jump * jump)
        total = total + weighted_mean(squares)
    total = jnp.sum(total, axis=(0, 1), keepdims=True)
    sum_ref[...] = jnp.broadcast_to(total[:, None], sum_ref.shape)


def hold(x):
    return pltpu.with_memory_space_constraint(x, pltpu.VMEM)


def work(count):
    shapes = [(64, count, 128), (64, count, 128), (7 * 16, count, 128), (16, count, 128)]
    return [pltpu.VMEM(shape, jnp.float32) for shape in shapes]


def estimate(updates):
    return pl.CostEstimate(
        flops=updates * 400_000_000, transcendentals=0, bytes_accessed=updates * 1_000_000
    )


def ring(axis, shift):
    count = lax.axis_size(axis)
    return [(i, (i + shift) % count) for i in range(count)]


def on_device(slab_starts, coarse_factor, blend_weight, blend_flags):
    f32 = jnp.float32
    vmem = pl.BlockSpec(memory_space=pltpu.VMEM)
    smem = pl.BlockSpec(memory_space=pltpu.SMEM)
    opening = slab_starts.reshape(64, 8, 128)
    slab = lax.axis_index(TM).astype(jnp.int32).reshape(1)
    raw = pl.BlockSpec(memory_space=pl.ANY)
    own = pl.pallas_call(
        join_kernel,
        out_shape=pltpu.VMEM((65, 8, 128), f32),
        in_specs=[raw] * 3,
        out_specs=vmem,
        scratch_shapes=[
            pltpu.VMEM((8, 128), f32),
            pltpu.VMEM((8, 128), jnp.int32),
            pltpu.SemaphoreType.DMA((3,)),
        ],
        name="join",
    )(opening, blend_weight, blend_flags)
    factor = hold(coarse_factor)
    left = lax.ppermute(own, SPACE, ring(SPACE, 1))
    right = lax.ppermute(own, SPACE, ring(SPACE, -1))
    own, left, right = hold(own), hold(left), hold(right)
    inner = pl.pallas_call(
        inner_kernel,
        out_shape=pltpu.VMEM((3, 64, 8, 128), f32),
        in_specs=[vmem],
        out_specs=vmem,
        scratch_shapes=work(16),
        cost_estimate=estimate(3),
        name="inner",
    )(own)
    strip = pl.pallas_call(
        right_kernel,
        out_shape=pltpu.VMEM((64, 8, 128), f32),
        in_specs=[vmem] * 3,
        out_specs=vmem,
        scratch_shapes=work(24) + [pltpu.VMEM((24, 128), f32)],
        cost_estimate=estimate(4),
        name="right",
    )(own, right, hold(inner))
    packed, plain = pl.pallas_call(
        fine_kernel,
        out_shape=(
            pltpu.VMEM((16, 4, 8, 128), f32),
            pltpu.VMEM((64, 8, 128), f32),
        ),
        in_specs=[smem] + [vmem] * 6,
        out_specs=[vmem] * 2,
        scratch_shapes=work(24) + [pltpu.VMEM((24, 128), f32)],
        cost_estimate=estimate(11),
        name="fine",
    )(slab, own, left, right, hold(inner), hold(strip), factor)
    gathered = lax.all_to_all(packed, TM, 0, 0)
    scanned = pl.pallas_call(
        scan_kernel,
        out_shape=pltpu.VMEM((16, 4, 8, 128), f32),
        in_specs=[smem] + [vmem] * 2,
        out_specs=vmem,
        name="scan",
    )(slab, hold(gathered), factor)
    starts = lax.all_to_all(scanned, TM, 0, 0)
    slab_end, partial_sums = pl.pallas_call(
        final_kernel,
        out_shape=(
            pltpu.VMEM((64, 8, 128), f32),
            pltpu.VMEM((16, 1, 128), f32),
        ),
        in_specs=[smem] + [vmem] * 4,
        out_specs=[vmem] * 2,
        name="final",
    )(slab, hold(starts), own, hold(plain), factor)
    shared = lax.all_to_all(partial_sums, SPACE, 0, 0)
    element_count = lax.axis_size(SPACE) * slab_starts.shape[4] * slab_starts.shape[5]
    jump_norm = jnp.sqrt(jnp.sum(shared[:, 0, 0]) / element_count)
    return (slab_end.reshape(slab_starts.shape), jump_norm[None])


def solution(mesh):
    split = Mesh(mesh.devices.reshape(8, 2, 4, 4), ("tm_0", "tm_1", "space_0", "space_1"))
    return jax.shard_map(
        on_device,
        mesh=split,
        in_specs=(
            P(TM, None, None, None, SPACE, None),
            P(None, SPACE, None),
            P(SPACE, None),
            P(SPACE, None),
        ),
        out_specs=(P(TM, None, None, None, SPACE, None), P(TM)),
        check_vma=False,
    )
```

```python
import math

import jax
import jax.numpy as jnp
import numpy as np
from jax import lax
from jax.experimental import pallas as pl
from jax.experimental.pallas import tpu as pltpu
from jax.sharding import Mesh
from jax.sharding import PartitionSpec as P

FSTEPS = 4
SPACE = ("space_0", "space_1")
TM = ("tm_0", "tm_1")
STEP = 0.003
WEIGHTS = (1.0 / 6.0, 5.0 / 6.0, 5.0 / 6.0, 1.0 / 6.0)


def derivative_table():
    inner = 1.0 / math.sqrt(5.0)
    points = np.array([-1.0, -inner, inner, 1.0])
    scales = np.array(
        [1.0 / np.prod([points[c] - points[o] for o in range(4) if o != c]) for c in range(4)]
    )
    table = np.zeros((4, 4))
    for r in range(4):
        for c in range(4):
            if r != c:
                table[r, c] = scales[c] / scales[r] / (points[r] - points[c])
        table[r, r] = -np.sum(table[r])
    return table


SPLIT = [[float(2.0 * WEIGHTS[i] * derivative_table()[i, k]) for k in range(4)] for i in range(4)]
EDGE = SPLIT[0][1]
SERIES = (105.0 / 52.5, 35.0 / 52.5, 21.0 / 52.5, 15.0 / 52.5)
BINARY = tuple(x / math.log(2.0) for x in SERIES)
BETA = 0.2 / math.log(2.0)
SOUND = math.sqrt(1.4 * BETA)


def log_parts(left, right, log_left, log_right, terms):
    total = left + right
    differ = right - left
    ratio = differ / total
    ratio = ratio * ratio
    nearly = ratio < 0.0001
    series = terms[0] + ratio * (terms[1] + ratio * (terms[2] + ratio * terms[3]))
    return jnp.where(nearly, total, differ), jnp.where(nearly, series, log_right - log_left)


def pair_flux(a, b, scale=None):
    top, bottom = log_parts(a["rho"], b["rho"], a["lrho"], b["lrho"], SERIES)
    mean = top / bottom
    top, bottom = log_parts(a["beta"], b["beta"], a["lbeta"], b["lbeta"], BINARY)
    thermal = bottom / top
    normal = a["n"] + b["n"]
    pressure = a["p"] + b["p"]
    cross = a["p"] * b["n"] + b["p"] * a["n"]
    if scale is not None:
        mean = mean * scale
        pressure = pressure * scale
        cross = cross * scale
    mass = mean * normal
    half = 0.5 * mass
    kinetic = a["n"] * b["n"] + a["t"] * b["t"] + thermal
    return (
        mass,
        half * normal + pressure,
        half * (a["t"] + b["t"]),
        half * kinetic + cross,
    )


def conserved(node):
    return (node["rho"], node["mn"], node["mt"], node["e"])


def face_flux(a, b, scale):
    central = pair_flux(a, b)
    speed = jnp.maximum(jnp.abs(a["n"]) + a["c"], jnp.abs(b["n"]) + b["c"])
    return tuple(
        scale * (c - speed * (ub - ua)) for c, ua, ub in zip(central, conserved(a), conserved(b), strict=True)
    )


def physical(node):
    return (
        node["mn"],
        node["mn"] * node["n"] + node["p"],
        node["mt"] * node["n"],
        node["n"] * (node["e"] + node["p"]),
    )


def line_walls(nodes, split_share, sub_share):
    pair = {}
    for i in range(4):
        for k in range(i + 1, 4):
            scale = None if k - i == 1 and i != 1 else SPLIT[i][k] / EDGE
            pair[i, k] = pair_flux(nodes[i], nodes[k], scale)
    own = [physical(node) for node in nodes]
    speeds = [jnp.abs(node["n"]) + node["c"] for node in nodes]
    out = [[], [], []]
    for v in range(4):
        far = pair[0, 3][v]
        left, right = far + pair[0, 2][v], far + pair[1, 3][v]
        walls = (
            left + pair[0, 1][v],
            (left + pair[1, 3][v]) + pair[1, 2][v],
            right + pair[2, 3][v],
        )
        for m in range(3):
            speed = jnp.maximum(speeds[m], speeds[m + 1])
            jump = conserved(nodes[m + 1])[v] - conserved(nodes[m])[v]
            sub = own[m][v] + own[m + 1][v] - speed * jump
            out[m].append(split_share * walls[m] + sub_share * sub)
    return out


ORDER = {1: (0, 1, 2, 3), 2: (0, 2, 1, 3)}
VX, VY, PR, LR, BE, LB, CS = range(7)


def at(v, i, j):
    return v * 16 + i * 4 + j


def rows(c, offset):
    start = c * 8 + offset
    if isinstance(c, int):
        return pl.ds(start, 8)
    return pl.ds(pl.multiple_of(c * 8, 8) + offset, 8)


def node_pass(src, prim, c):
    here = rows(c, 0)
    for n in range(16):
        rho = src[n, here, :]
        inv = 1.0 / rho
        mx = src[16 + n, here, :]
        my = src[32 + n, here, :]
        vx = mx * inv
        vy = my * inv
        p = 0.4 * src[48 + n, here, :] - 0.2 * (mx * vx + my * vy)
        beta = BETA * rho / p
        prim[VX * 16 + n, here, :] = vx
        prim[VY * 16 + n, here, :] = vy
        prim[PR * 16 + n, here, :] = p
        prim[LR * 16 + n, here, :] = jnp.log(rho)
        prim[BE * 16 + n, here, :] = beta
        prim[LB * 16 + n, here, :] = jnp.log2(beta)
        prim[CS * 16 + n, here, :] = SOUND * lax.rsqrt(beta)


def node(src, prim, i, j, here, axis):
    n = i * 4 + j
    normal, along = (VX, VY) if axis == 1 else (VY, VX)
    order = ORDER[axis]
    return {
        "rho": src[n, here, :],
        "mn": src[order[1] * 16 + n, here, :],
        "mt": src[order[2] * 16 + n, here, :],
        "e": src[48 + n, here, :],
        "n": prim[normal * 16 + n, here, :],
        "t": prim[along * 16 + n, here, :],
        "p": prim[PR * 16 + n, here, :],
        "lrho": prim[LR * 16 + n, here, :],
        "beta": prim[BE * 16 + n, here, :],
        "lbeta": prim[LB * 16 + n, here, :],
        "c": prim[CS * 16 + n, here, :],
    }


def face_pass(src, prim, faces, c, scale):
    for j in range(4):
        lower = node(src, prim, 3, j, rows(c, 0), 1)
        flux = face_flux(lower, node(src, prim, 0, j, rows(c, 1), 1), scale)
        for v in range(4):
            faces[j * 4 + v, rows(c, 0), :] = flux[v]


def update_pass(src, dst, prim, faces, c, blend, second, right):
    here = rows(c, 1)
    there, start_rows = (rows(c, 2), rows(c, 0)) if right else (rows(c, 0), rows(c, 2))
    scale = (0.5 if second else 1.0) * STEP / WEIGHTS[1]
    sub_share = scale * blend
    split_share = (scale - sub_share) * EDGE
    for j in range(4):
        nodes = [node(src, prim, i, j, here, 1) for i in range(4)]
        walls = line_walls(nodes, split_share, sub_share)
        for v in range(4):
            column = [faces[j * 4 + v, rows(c, 0), :]]
            column += [walls[m][v] for m in range(3)]
            column += [faces[j * 4 + v, here, :]]
            for i in range(4):
                k = at(v, i, j)
                change = column[i + 1] - column[i]
                if i in (0, 3):
                    change = (WEIGHTS[1] / WEIGHTS[0]) * change
                if second:
                    start = 0.5 * (dst[k, start_rows, :] + src[k, here, :])
                else:
                    start = src[k, here, :]
                dst[k, there, :] = start - change
    for i in range(4):
        nodes = [node(src, prim, i, j, here, 2) for j in range(4)]
        behind = {key: pltpu.roll(x, 1, 1) for key, x in nodes[3].items()}
        low = face_flux(behind, nodes[0], scale)
        high = tuple(pltpu.roll(x, 127, 1) for x in low)
        walls = line_walls(nodes, split_share, sub_share)
        for q in range(4):
            v = ORDER[2][q]
            column = [low[q]] + [walls[m][q] for m in range(3)] + [high[q]]
            for j in range(4):
                k = at(v, i, j)
                change = column[j + 1] - column[j]
                if j in (0, 3):
                    change = (WEIGHTS[1] / WEIGHTS[0]) * change
                dst[k, there, :] = dst[k, there, :] - change


def loop(count, body):
    if isinstance(count, int) and count == 1:
        body(0)
        return

    def step(c, carry):
        body(c)
        return carry

    lax.fori_loop(0, count, step, 0)


def stage(src, dst, work, second, right, chunks, blend_at, updates):
    prim, faces = work
    scale = (0.5 if second else 1.0) * STEP / WEIGHTS[1]
    loop(chunks, lambda c: node_pass(src, prim, c))
    loop(chunks, lambda c: face_pass(src, prim, faces, c, scale))
    loop(
        updates, lambda c: update_pass(src, dst, prim, faces, c, blend_at(c), second, right)
    )


def join_kernel(opening_ref, weight_ref, flags_ref, own_ref, weight, flags, sems):
    copies = [
        pltpu.make_async_copy(opening_ref, own_ref.at[pl.ds(0, 64)], sems.at[0]),
        pltpu.make_async_copy(weight_ref, weight, sems.at[1]),
        pltpu.make_async_copy(flags_ref, flags, sems.at[2]),
    ]
    for copy in copies:
        copy.start()
    copies[1].wait()
    copies[2].wait()
    own_ref[64] = flags[...].astype(jnp.float32) * weight[...]
    copies[0].wait()


def inner_kernel(own_ref, inner_ref, base, mid, prim, faces):
    for k in range(64):
        base[k, 0:8, :] = own_ref[k]
    blend = own_ref[64]
    for s in range(1, 4):
        second = s == 2
        src, dst = (mid, base) if second else (base, mid)
        shifted = pltpu.roll(blend, 8 - s, 0)
        stage(src, dst, (prim, faces), second, False, 1, lambda c: shifted, 1)
        for k in range(64):
            inner_ref[s - 1, k] = dst[k, 0:8, :]


def right_kernel(own_ref, right_ref, inner_ref, out_ref, base, mid, prim, faces, blend_ref):
    for k in range(64):
        base[k, 0:2, :] = own_ref[k, 6:8, :]
        base[k, 2:10, :] = right_ref[k]
    blend_ref[0:8, :] = own_ref[64]
    blend_ref[8:16, :] = right_ref[64]

    def fill(dst, s):
        def one(k, carry):
            dst[k, 0:2, :] = inner_ref[s - 1, k, pl.ds(6 - 2 * s, 2), :]
            return carry

        lax.fori_loop(0, 64, one, 0, unroll=16)

    def time_step(t, carry):
        for second in (False, True):
            s = 2 * t + (2 if second else 1)
            src, dst = (mid, base) if second else (base, mid)
            blend_at = lambda c, s=s: blend_ref[pl.ds(8 - s, 8), :]
            stage(src, dst, (prim, faces), second, True, 2, blend_at, 1)
            fill(dst, jnp.minimum(s, 3))
        return carry

    lax.fori_loop(0, 2, time_step, 0)
    for k in range(64):
        out_ref[k] = base[k, 2:10, :]


def fine_kernel(
    slab_ref, own_ref, left_ref, right_ref, inner_ref, strip_ref, factor_ref,
    sent_ref, plain_ref, base, mid, prim, faces, blend_ref,
):
    for k in range(64):
        base[k, 0:8, :] = left_ref[k]
        base[k, 8:10, :] = own_ref[k, 0:2, :]
    blend_ref[0:8, :] = left_ref[64]
    blend_ref[8:16, :] = own_ref[64]
    blend_ref[16:24, :] = right_ref[64]

    def fill(dst, s):
        @pl.when(s < 4)
        def _():
            def one(k, carry):
                dst[k, 8:10, :] = inner_ref[s - 1, k, 0:2, :]
                return carry

            lax.fori_loop(0, 64, one, 0, unroll=16)

        @pl.when(s == 4)
        def _():
            def one(k, carry):
                dst[k, 8:16, :] = strip_ref[k]
                return carry

            lax.fori_loop(0, 64, one, 0, unroll=16)

    def time_step(t, carry):
        for second in (False, True):
            s = 2 * t + (2 if second else 1)
            src, dst = (mid, base) if second else (base, mid)
            blend_at = lambda c, s=s: blend_ref[pl.ds(8 * c + s, 8), :]
            updates = jnp.where((s > 4) & (s < 8), 2, 1)
            stage(src, dst, (prim, faces), second, False, 2, blend_at, updates)
            fill(dst, s)
        return carry

    lax.fori_loop(0, FSTEPS, time_step, 0)

    later = jnp.where(slab_ref[0] == 0, 0.0, 1.0).astype(jnp.float32)
    for v in range(4):
        factor = factor_ref[v]
        mean = weighted_mean([own_ref[v * 16 + n] for n in range(16)])
        for n in range(16):
            k = v * 16 + n
            guess = mean + factor * (own_ref[k] - mean)
            plain_ref[k] = base[k, 0:8, :] - later * guess
    other = 32 * (1 - (slab_ref[0] & 1))
    for k in range(32):
        sent_ref[k] = plain_ref[other + k]


def weighted_mean(values):
    total = None
    for n, x in enumerate(values):
        term = (WEIGHTS[n // 4] * WEIGHTS[n % 4] / 4.0) * x
        total = term if total is None else total + term
    return total


def exchange(blocks):
    group = lax.broadcasted_iota(jnp.int32, (8, 128), 0) // 2
    out = []
    for q in range(4):
        piece = None
        for j in range(4):
            shift = (2 * (j - q)) % 8
            moved = pltpu.roll(blocks[j], shift, 0) if shift else blocks[j]
            piece = moved if piece is None else jnp.where(group == j, moved, piece)
        out.append(piece)
    return out


def chip_parts(slab_ref, plain_ref, got_ref, w):
    core = slab_ref[0] & 1
    even_here = core == 0
    evens, odds = [], []
    for n in range(16):
        mine, theirs = plain_ref[32 * core + 16 * w + n], got_ref[16 * w + n]
        evens.append(jnp.where(even_here, mine, theirs))
        odds.append(jnp.where(even_here, theirs, mine))
    return core, evens, odds


def pair_kernel(slab_ref, plain_ref, got_ref, factor_ref, out_ref):
    for w in range(2):
        core, evens, odds = chip_parts(slab_ref, plain_ref, got_ref, w)
        factor = factor_ref[2 * core + w]
        mean = weighted_mean(evens)
        both = [mean + factor * (x - mean) + y for x, y in zip(evens, odds, strict=True)]
        for i in range(4):
            for q, piece in enumerate(exchange(both[4 * i : 4 * i + 4])):
                out_ref[w * 4 + q, i] = piece


def scan_kernel(slab_ref, given_ref, factor_ref, out_ref):
    slab = slab_ref[0]
    chip = lax.shift_right_logical(slab, 1)
    var = 2 * (slab & 1) + lax.shift_right_logical(chip, 2)
    first = 2 * (chip & 3)
    row = lax.broadcasted_iota(jnp.int32, (8, 128), 0)
    even = jnp.broadcast_to(factor_ref[var, pl.ds(first, 1), :], (8, 128))
    odd = jnp.broadcast_to(factor_ref[var, pl.ds(first + 1, 1), :], (8, 128))
    factor = jnp.where((row & 1) == 0, even, odd)
    factor = factor * factor
    outer = (row < 2) | (row >= 6)
    low = jnp.where(outer, WEIGHTS[0], WEIGHTS[1]).astype(jnp.float32) * (WEIGHTS[0] / 4.0)
    high = jnp.where(outer, WEIGHTS[0], WEIGHTS[1]).astype(jnp.float32) * (WEIGHTS[1] / 4.0)
    state = [given_ref[0, i] for i in range(4)]
    for i in range(4):
        out_ref[0, i] = state[i]
    for n in range(1, 8):
        for i in range(4):
            out_ref[n, i] = state[i]
        if n == 7:
            break
        part = (state[0] + state[3]) * low + (state[1] + state[2]) * high
        part = part + pltpu.roll(part, 4, 0)
        mean = part + pltpu.roll(part, 2, 0)
        state = [mean + factor * (state[i] - mean) + given_ref[n, i] for i in range(4)]


def spread_kernel(slab_ref, pieces_ref, plain_ref, got_ref, factor_ref, kept_ref, sent_ref):
    later = jnp.where(slab_ref[0] < 2, 0.0, 1.0).astype(jnp.float32)
    for w in range(2):
        core, evens, _ = chip_parts(slab_ref, plain_ref, got_ref, w)
        factor = factor_ref[2 * core + w]
        starts = []
        for i in range(4):
            starts += exchange([pieces_ref[w * 4 + q, i] for q in range(4)])
        mean = weighted_mean(starts)
        for n in range(16):
            second = later * (mean + factor * (starts[n] - mean)) + evens[n]
            kept_ref[16 * w + n] = jnp.where(core == 0, starts[n], second)
            sent_ref[16 * w + n] = jnp.where(core == 0, second, starts[n])


def final_kernel(
    slab_ref, kept_ref, got_ref, own_ref, plain_ref, factor_ref, end_ref, sum_ref, starts_ref
):
    later = jnp.where(slab_ref[0] == 0, 0.0, 1.0).astype(jnp.float32)
    here = 32 * (slab_ref[0] & 1)
    for k in range(32):
        starts_ref[here + k] = kept_ref[k]
        starts_ref[32 - here + k] = got_ref[k]
    total = jnp.zeros((8, 128), jnp.float32)
    for v in range(4):
        factor = factor_ref[v]
        starts = [starts_ref[v * 16 + n] for n in range(16)]
        mean = weighted_mean(starts)
        squares = []
        for n in range(16):
            k = v * 16 + n
            end_ref[k] = later * (mean + factor * (starts[n] - mean)) + plain_ref[k]
            jump = later * (starts[n] - own_ref[k])
            squares.append(jump * jump)
        total = total + weighted_mean(squares)
    total = jnp.sum(total, axis=(0, 1), keepdims=True)
    sum_ref[...] = jnp.broadcast_to(total[:, None], sum_ref.shape)


def hold(x):
    return pltpu.with_memory_space_constraint(x, pltpu.VMEM)


def work(count):
    shapes = [(64, count, 128), (64, count, 128), (7 * 16, count, 128), (16, count, 128)]
    return [pltpu.VMEM(shape, jnp.float32) for shape in shapes]


def estimate(updates):
    return pl.CostEstimate(
        flops=updates * 400_000_000, transcendentals=0, bytes_accessed=updates * 1_000_000
    )


def ring(axis, shift):
    count = lax.axis_size(axis)
    return [(i, (i + shift) % count) for i in range(count)]


def on_device(slab_starts, coarse_factor, blend_weight, blend_flags):
    f32 = jnp.float32
    vmem = pl.BlockSpec(memory_space=pltpu.VMEM)
    smem = pl.BlockSpec(memory_space=pltpu.SMEM)
    opening = slab_starts.reshape(64, 8, 128)
    slab = lax.axis_index(TM).astype(jnp.int32).reshape(1)
    raw = pl.BlockSpec(memory_space=pl.ANY)
    own = pl.pallas_call(
        join_kernel,
        out_shape=pltpu.VMEM((65, 8, 128), f32),
        in_specs=[raw] * 3,
        out_specs=vmem,
        scratch_shapes=[
            pltpu.VMEM((8, 128), f32),
            pltpu.VMEM((8, 128), jnp.int32),
            pltpu.SemaphoreType.DMA((3,)),
        ],
        name="join",
    )(opening, blend_weight, blend_flags)
    factor = hold(coarse_factor)
    left = lax.ppermute(own, SPACE, ring(SPACE, 1))
    right = lax.ppermute(own, SPACE, ring(SPACE, -1))
    own, left, right = hold(own), hold(left), hold(right)
    inner = pl.pallas_call(
        inner_kernel,
        out_shape=pltpu.VMEM((3, 64, 8, 128), f32),
        in_specs=[vmem],
        out_specs=vmem,
        scratch_shapes=work(16),
        cost_estimate=estimate(3),
        name="inner",
    )(own)
    strip = pl.pallas_call(
        right_kernel,
        out_shape=pltpu.VMEM((64, 8, 128), f32),
        in_specs=[vmem] * 3,
        out_specs=vmem,
        scratch_shapes=work(24) + [pltpu.VMEM((24, 128), f32)],
        cost_estimate=estimate(4),
        name="right",
    )(own, right, hold(inner))
    sent, plain = pl.pallas_call(
        fine_kernel,
        out_shape=(
            pltpu.VMEM((32, 8, 128), f32),
            pltpu.VMEM((64, 8, 128), f32),
        ),
        in_specs=[smem] + [vmem] * 6,
        out_specs=[vmem] * 2,
        scratch_shapes=work(24) + [pltpu.VMEM((24, 128), f32)],
        cost_estimate=estimate(11),
        name="fine",
    )(slab, own, left, right, hold(inner), hold(strip), factor)
    plain = hold(plain)
    got = hold(lax.ppermute(sent, TM[1], ring(TM[1], 1)))
    both = pl.pallas_call(
        pair_kernel,
        out_shape=pltpu.VMEM((8, 4, 8, 128), f32),
        in_specs=[smem] + [vmem] * 3,
        out_specs=vmem,
        name="pair",
    )(slab, plain, got, factor)
    gathered = lax.all_to_all(both, TM[0], 0, 0)
    scanned = pl.pallas_call(
        scan_kernel,
        out_shape=pltpu.VMEM((8, 4, 8, 128), f32),
        in_specs=[smem] + [vmem] * 2,
        out_specs=vmem,
        name="scan",
    )(slab, hold(gathered), factor)
    pieces = lax.all_to_all(scanned, TM[0], 0, 0)
    kept, given = pl.pallas_call(
        spread_kernel,
        out_shape=(pltpu.VMEM((32, 8, 128), f32), pltpu.VMEM((32, 8, 128), f32)),
        in_specs=[smem] + [vmem] * 4,
        out_specs=[vmem] * 2,
        name="spread",
    )(slab, hold(pieces), plain, got, factor)
    arrived = lax.ppermute(given, TM[1], ring(TM[1], 1))
    slab_end, partial_sums = pl.pallas_call(
        final_kernel,
        out_shape=(
            pltpu.VMEM((64, 8, 128), f32),
            pltpu.VMEM((16, 1, 128), f32),
        ),
        in_specs=[smem] + [vmem] * 5,
        out_specs=[vmem] * 2,
        scratch_shapes=[pltpu.VMEM((64, 8, 128), f32)],
        name="final",
    )(slab, hold(kept), hold(arrived), own, plain, factor)
    shared = lax.all_to_all(partial_sums, SPACE, 0, 0)
    element_count = lax.axis_size(SPACE) * slab_starts.shape[4] * slab_starts.shape[5]
    jump_norm = jnp.sqrt(jnp.sum(shared[:, 0, 0]) / element_count)
    return (slab_end.reshape(slab_starts.shape), jump_norm[None])


def solution(mesh):
    split = Mesh(mesh.devices.reshape(8, 2, 4, 4), ("tm_0", "tm_1", "space_0", "space_1"))
    return jax.shard_map(
        on_device,
        mesh=split,
        in_specs=(
            P(TM, None, None, None, SPACE, None),
            P(None, SPACE, None),
            P(SPACE, None),
            P(SPACE, None),
        ),
        out_specs=(P(TM, None, None, None, SPACE, None), P(TM)),
        check_vma=False,
    )
```

```python
import math

import jax
import jax.numpy as jnp
import numpy as np
from jax import lax
from jax.experimental import pallas as pl
from jax.experimental.pallas import tpu as pltpu
from jax.sharding import Mesh
from jax.sharding import PartitionSpec as P

FSTEPS = 4
SPACE = ("space_0", "space_1")
TM = ("tm_0", "tm_1")
PLANE = ("tm_1", "space_0", "space_1")
STEP = 0.003
WEIGHTS = (1.0 / 6.0, 5.0 / 6.0, 5.0 / 6.0, 1.0 / 6.0)


def derivative_table():
    inner = 1.0 / math.sqrt(5.0)
    points = np.array([-1.0, -inner, inner, 1.0])
    scales = np.array(
        [1.0 / np.prod([points[c] - points[o] for o in range(4) if o != c]) for c in range(4)]
    )
    table = np.zeros((4, 4))
    for r in range(4):
        for c in range(4):
            if r != c:
                table[r, c] = scales[c] / scales[r] / (points[r] - points[c])
        table[r, r] = -np.sum(table[r])
    return table


SPLIT = [[float(2.0 * WEIGHTS[i] * derivative_table()[i, k]) for k in range(4)] for i in range(4)]
EDGE = SPLIT[0][1]
SERIES = (105.0 / 52.5, 35.0 / 52.5, 21.0 / 52.5, 15.0 / 52.5)
BINARY = tuple(x / math.log(2.0) for x in SERIES)
BETA = 0.2 / math.log(2.0)
SOUND = math.sqrt(1.4 * BETA)


def log_parts(left, right, log_left, log_right, terms):
    total = left + right
    differ = right - left
    ratio = differ / total
    ratio = ratio * ratio
    nearly = ratio < 0.0001
    series = terms[0] + ratio * (terms[1] + ratio * (terms[2] + ratio * terms[3]))
    return jnp.where(nearly, total, differ), jnp.where(nearly, series, log_right - log_left)


def pair_flux(a, b, scale=None):
    top, bottom = log_parts(a["rho"], b["rho"], a["lrho"], b["lrho"], SERIES)
    mean = top / bottom
    top, bottom = log_parts(a["beta"], b["beta"], a["lbeta"], b["lbeta"], BINARY)
    thermal = bottom / top
    normal = a["n"] + b["n"]
    pressure = a["p"] + b["p"]
    cross = a["p"] * b["n"] + b["p"] * a["n"]
    if scale is not None:
        mean = mean * scale
        pressure = pressure * scale
        cross = cross * scale
    mass = mean * normal
    half = 0.5 * mass
    kinetic = a["n"] * b["n"] + a["t"] * b["t"] + thermal
    return (
        mass,
        half * normal + pressure,
        half * (a["t"] + b["t"]),
        half * kinetic + cross,
    )


def conserved(node):
    return (node["rho"], node["mn"], node["mt"], node["e"])


def face_flux(a, b, scale):
    central = pair_flux(a, b)
    speed = jnp.maximum(jnp.abs(a["n"]) + a["c"], jnp.abs(b["n"]) + b["c"])
    return tuple(
        scale * (c - speed * (ub - ua)) for c, ua, ub in zip(central, conserved(a), conserved(b), strict=True)
    )


def physical(node):
    return (
        node["mn"],
        node["mn"] * node["n"] + node["p"],
        node["mt"] * node["n"],
        node["n"] * (node["e"] + node["p"]),
    )


def line_walls(nodes, split_share, sub_share):
    pair = {}
    for i in range(4):
        for k in range(i + 1, 4):
            scale = None if k - i == 1 and i != 1 else SPLIT[i][k] / EDGE
            pair[i, k] = pair_flux(nodes[i], nodes[k], scale)
    own = [physical(node) for node in nodes]
    speeds = [jnp.abs(node["n"]) + node["c"] for node in nodes]
    out = [[], [], []]
    for v in range(4):
        far = pair[0, 3][v]
        left, right = far + pair[0, 2][v], far + pair[1, 3][v]
        walls = (
            left + pair[0, 1][v],
            (left + pair[1, 3][v]) + pair[1, 2][v],
            right + pair[2, 3][v],
        )
        for m in range(3):
            speed = jnp.maximum(speeds[m], speeds[m + 1])
            jump = conserved(nodes[m + 1])[v] - conserved(nodes[m])[v]
            sub = own[m][v] + own[m + 1][v] - speed * jump
            out[m].append(split_share * walls[m] + sub_share * sub)
    return out


ORDER = {1: (0, 1, 2, 3), 2: (0, 2, 1, 3)}
VX, VY, PR, LR, BE, LB, CS = range(7)


def at(v, i, j):
    return v * 16 + i * 4 + j


def rows(c, offset):
    start = c * 8 + offset
    if isinstance(c, int):
        return pl.ds(start, 8)
    return pl.ds(pl.multiple_of(c * 8, 8) + offset, 8)


def node_pass(src, prim, c):
    here = rows(c, 0)
    for n in range(16):
        rho = src[n, here, :]
        inv = 1.0 / rho
        mx = src[16 + n, here, :]
        my = src[32 + n, here, :]
        vx = mx * inv
        vy = my * inv
        p = 0.4 * src[48 + n, here, :] - 0.2 * (mx * vx + my * vy)
        beta = BETA * rho / p
        prim[VX * 16 + n, here, :] = vx
        prim[VY * 16 + n, here, :] = vy
        prim[PR * 16 + n, here, :] = p
        prim[LR * 16 + n, here, :] = jnp.log(rho)
        prim[BE * 16 + n, here, :] = beta
        prim[LB * 16 + n, here, :] = jnp.log2(beta)
        prim[CS * 16 + n, here, :] = SOUND * lax.rsqrt(beta)


def node(src, prim, i, j, here, axis):
    n = i * 4 + j
    normal, along = (VX, VY) if axis == 1 else (VY, VX)
    order = ORDER[axis]
    return {
        "rho": src[n, here, :],
        "mn": src[order[1] * 16 + n, here, :],
        "mt": src[order[2] * 16 + n, here, :],
        "e": src[48 + n, here, :],
        "n": prim[normal * 16 + n, here, :],
        "t": prim[along * 16 + n, here, :],
        "p": prim[PR * 16 + n, here, :],
        "lrho": prim[LR * 16 + n, here, :],
        "beta": prim[BE * 16 + n, here, :],
        "lbeta": prim[LB * 16 + n, here, :],
        "c": prim[CS * 16 + n, here, :],
    }


def face_pass(src, prim, faces, c, scale):
    for j in range(4):
        lower = node(src, prim, 3, j, rows(c, 0), 1)
        flux = face_flux(lower, node(src, prim, 0, j, rows(c, 1), 1), scale)
        for v in range(4):
            faces[j * 4 + v, rows(c, 0), :] = flux[v]


def update_pass(src, dst, prim, faces, c, blend, second, side):
    here = rows(c, 1)
    there, start_rows = rows(c, 2 * side), rows(c, 2 - 2 * side)
    scale = (0.5 if second else 1.0) * STEP / WEIGHTS[1]
    sub_share = scale * blend
    split_share = (scale - sub_share) * EDGE
    for j in range(4):
        nodes = [node(src, prim, i, j, here, 1) for i in range(4)]
        walls = line_walls(nodes, split_share, sub_share)
        for v in range(4):
            column = [faces[j * 4 + v, rows(c, 0), :]]
            column += [walls[m][v] for m in range(3)]
            column += [faces[j * 4 + v, here, :]]
            for i in range(4):
                k = at(v, i, j)
                change = column[i + 1] - column[i]
                if i in (0, 3):
                    change = (WEIGHTS[1] / WEIGHTS[0]) * change
                if second:
                    start = 0.5 * (dst[k, start_rows, :] + src[k, here, :])
                else:
                    start = src[k, here, :]
                dst[k, there, :] = start - change
    for i in range(4):
        nodes = [node(src, prim, i, j, here, 2) for j in range(4)]
        behind = {key: pltpu.roll(x, 1, 1) for key, x in nodes[3].items()}
        low = face_flux(behind, nodes[0], scale)
        high = tuple(pltpu.roll(x, 127, 1) for x in low)
        walls = line_walls(nodes, split_share, sub_share)
        for q in range(4):
            v = ORDER[2][q]
            column = [low[q]] + [walls[m][q] for m in range(3)] + [high[q]]
            for j in range(4):
                k = at(v, i, j)
                change = column[j + 1] - column[j]
                if j in (0, 3):
                    change = (WEIGHTS[1] / WEIGHTS[0]) * change
                dst[k, there, :] = dst[k, there, :] - change


def loop(count, body):
    if isinstance(count, int) and count == 1:
        body(0)
        return

    def step(c, carry):
        body(c)
        return carry

    lax.fori_loop(0, count, step, 0)


def stage(src, dst, work, second, side, chunks, blend_at, updates):
    prim, faces = work
    scale = (0.5 if second else 1.0) * STEP / WEIGHTS[1]
    loop(chunks, lambda c: node_pass(src, prim, c))
    loop(chunks, lambda c: face_pass(src, prim, faces, c, scale))
    loop(
        updates, lambda c: update_pass(src, dst, prim, faces, c, blend_at(c), second, side)
    )


def join_kernel(opening_ref, weight_ref, flags_ref, own_ref, weight, flags, sems):
    copies = [
        pltpu.make_async_copy(opening_ref, own_ref.at[pl.ds(0, 64)], sems.at[0]),
        pltpu.make_async_copy(weight_ref, weight, sems.at[1]),
        pltpu.make_async_copy(flags_ref, flags, sems.at[2]),
    ]
    for copy in copies:
        copy.start()
    copies[1].wait()
    copies[2].wait()
    own_ref[64] = flags[...].astype(jnp.float32) * weight[...]
    copies[0].wait()


def inner_kernel(own_ref, inner_ref, base, mid, prim, faces):
    for k in range(64):
        base[k, 0:8, :] = own_ref[k]
    blend = own_ref[64]
    for s in range(1, 4):
        second = s == 2
        src, dst = (mid, base) if second else (base, mid)
        shifted = pltpu.roll(blend, 8 - s, 0)
        stage(src, dst, (prim, faces), second, 0, 1, lambda c: shifted, 1)
        for k in range(64):
            inner_ref[s - 1, k] = dst[k, 0:8, :]


def begin_strip(base, own_ref, block_ref, side):
    for k in range(64):
        base[k, pl.ds(2 * side, 8), :] = block_ref[k]
        base[k, pl.ds(8 - 8 * side, 2), :] = own_ref[k, pl.ds(6 * side, 2), :]


def continue_strip(dst, inner_ref, s, side):
    def one(k, carry):
        dst[k, pl.ds(8 - 8 * side, 2), :] = inner_ref[s - 1, k, pl.ds(side * (6 - 2 * s), 2), :]
        return carry

    lax.fori_loop(0, 64, one, 0, unroll=16)


def strip_kernel(
    slab_ref, own_ref, block_ref, inner_ref, out_ref, base, mid, prim, faces, blend_ref
):
    side = slab_ref[0] & 1
    begin_strip(base, own_ref, block_ref, side)
    blend_ref[0:8, :] = block_ref[64]
    blend_ref[8:16, :] = own_ref[64]
    blend_ref[16:24, :] = block_ref[64]

    def time_step(t, carry):
        for second in (False, True):
            s = 2 * t + (2 if second else 1)
            src, dst = (mid, base) if second else (base, mid)
            blend_at = lambda c, s=s: blend_ref[pl.ds(s + side * (16 - 2 * s), 8), :]
            stage(src, dst, (prim, faces), second, side, 2, blend_at, 1)
            continue_strip(dst, inner_ref, jnp.minimum(s, 3), side)
        return carry

    lax.fori_loop(0, 2, time_step, 0)
    for k in range(64):
        out_ref[k] = base[k, pl.ds(2 * side, 8), :]


def fine_kernel(
    slab_ref, own_ref, first_ref, block_ref, inner_ref, strip_ref, factor_ref,
    sent_ref, plain_ref, base, mid, prim, faces, blend_ref,
):
    other_side = slab_ref[0] & 1
    side = 1 - other_side
    begin_strip(base, own_ref, block_ref, side)
    blend_ref[pl.ds(16 * other_side, 8), :] = first_ref[64]
    blend_ref[8:16, :] = own_ref[64]
    blend_ref[pl.ds(16 * side, 8), :] = block_ref[64]

    def fill(dst, s):
        @pl.when(s < 4)
        def _():
            continue_strip(dst, inner_ref, s, side)

        @pl.when(s == 4)
        def _():
            def one(k, carry):
                strip = dst[k, pl.ds(2 * side, 8), :]
                dst[k, pl.ds(8 * side, 8), :] = strip
                dst[k, pl.ds(8 - 8 * side, 8), :] = strip_ref[k]
                return carry

            lax.fori_loop(0, 64, one, 0, unroll=16)

    def time_step(t, carry):
        now = jnp.where(t < 2, side, 0)
        for second in (False, True):
            s = 2 * t + (2 if second else 1)
            src, dst = (mid, base) if second else (base, mid)
            blend_at = lambda c, s=s: blend_ref[pl.ds(8 * c + s + now * (16 - 2 * s), 8), :]
            updates = jnp.where((s > 4) & (s < 8), 2, 1)
            stage(src, dst, (prim, faces), second, now, 2, blend_at, updates)
            fill(dst, s)
        return carry

    lax.fori_loop(0, FSTEPS, time_step, 0)

    later = jnp.where(slab_ref[0] == 0, 0.0, 1.0).astype(jnp.float32)
    for v in range(4):
        factor = factor_ref[v]
        mean = weighted_mean([own_ref[v * 16 + n] for n in range(16)])
        for n in range(16):
            k = v * 16 + n
            guess = mean + factor * (own_ref[k] - mean)
            plain_ref[k] = base[k, 0:8, :] - later * guess
    other = 32 * (1 - (slab_ref[0] & 1))
    for k in range(32):
        sent_ref[k] = plain_ref[other + k]


def weighted_mean(values):
    total = None
    for n, x in enumerate(values):
        term = (WEIGHTS[n // 4] * WEIGHTS[n % 4] / 4.0) * x
        total = term if total is None else total + term
    return total


def exchange(blocks):
    group = lax.broadcasted_iota(jnp.int32, (8, 128), 0) // 2
    out = []
    for q in range(4):
        piece = None
        for j in range(4):
            shift = (2 * (j - q)) % 8
            moved = pltpu.roll(blocks[j], shift, 0) if shift else blocks[j]
            piece = moved if piece is None else jnp.where(group == j, moved, piece)
        out.append(piece)
    return out


def chip_parts(slab_ref, plain_ref, got_ref, w):
    core = slab_ref[0] & 1
    even_here = core == 0
    evens, odds = [], []
    for n in range(16):
        mine, theirs = plain_ref[32 * core + 16 * w + n], got_ref[16 * w + n]
        evens.append(jnp.where(even_here, mine, theirs))
        odds.append(jnp.where(even_here, theirs, mine))
    return core, evens, odds


def pair_kernel(slab_ref, plain_ref, got_ref, factor_ref, out_ref):
    for w in range(2):
        core, evens, odds = chip_parts(slab_ref, plain_ref, got_ref, w)
        factor = factor_ref[2 * core + w]
        mean = weighted_mean(evens)
        both = [mean + factor * (x - mean) + y for x, y in zip(evens, odds, strict=True)]
        for i in range(4):
            for q, piece in enumerate(exchange(both[4 * i : 4 * i + 4])):
                out_ref[w * 4 + q, i] = piece


def scan_kernel(slab_ref, given_ref, factor_ref, out_ref):
    slab = slab_ref[0]
    chip = lax.shift_right_logical(slab, 1)
    var = 2 * (slab & 1) + lax.shift_right_logical(chip, 2)
    first = 2 * (chip & 3)
    row = lax.broadcasted_iota(jnp.int32, (8, 128), 0)
    even = jnp.broadcast_to(factor_ref[var, pl.ds(first, 1), :], (8, 128))
    odd = jnp.broadcast_to(factor_ref[var, pl.ds(first + 1, 1), :], (8, 128))
    factor = jnp.where((row & 1) == 0, even, odd)
    factor = factor * factor
    outer = (row < 2) | (row >= 6)
    low = jnp.where(outer, WEIGHTS[0], WEIGHTS[1]).astype(jnp.float32) * (WEIGHTS[0] / 4.0)
    high = jnp.where(outer, WEIGHTS[0], WEIGHTS[1]).astype(jnp.float32) * (WEIGHTS[1] / 4.0)
    state = [given_ref[0, i] for i in range(4)]
    for i in range(4):
        out_ref[0, i] = state[i]
    for n in range(1, 8):
        for i in range(4):
            out_ref[n, i] = state[i]
        if n == 7:
            break
        part = (state[0] + state[3]) * low + (state[1] + state[2]) * high
        part = part + pltpu.roll(part, 4, 0)
        mean = part + pltpu.roll(part, 2, 0)
        state = [mean + factor * (state[i] - mean) + given_ref[n, i] for i in range(4)]


def spread_kernel(slab_ref, pieces_ref, plain_ref, got_ref, factor_ref, kept_ref, sent_ref):
    later = jnp.where(slab_ref[0] < 2, 0.0, 1.0).astype(jnp.float32)
    for w in range(2):
        core, evens, _ = chip_parts(slab_ref, plain_ref, got_ref, w)
        factor = factor_ref[2 * core + w]
        starts = []
        for i in range(4):
            starts += exchange([pieces_ref[w * 4 + q, i] for q in range(4)])
        mean = weighted_mean(starts)
        for n in range(16):
            second = later * (mean + factor * (starts[n] - mean)) + evens[n]
            kept_ref[16 * w + n] = jnp.where(core == 0, starts[n], second)
            sent_ref[16 * w + n] = jnp.where(core == 0, second, starts[n])


def final_kernel(
    slab_ref, kept_ref, got_ref, own_ref, plain_ref, factor_ref, end_ref, sum_ref, starts_ref
):
    later = jnp.where(slab_ref[0] == 0, 0.0, 1.0).astype(jnp.float32)
    here = 32 * (slab_ref[0] & 1)
    for k in range(32):
        starts_ref[here + k] = kept_ref[k]
        starts_ref[32 - here + k] = got_ref[k]
    total = jnp.zeros((8, 128), jnp.float32)
    for v in range(4):
        factor = factor_ref[v]
        starts = [starts_ref[v * 16 + n] for n in range(16)]
        mean = weighted_mean(starts)
        squares = []
        for n in range(16):
            k = v * 16 + n
            end_ref[k] = later * (mean + factor * (starts[n] - mean)) + plain_ref[k]
            jump = later * (starts[n] - own_ref[k])
            squares.append(jump * jump)
        total = total + weighted_mean(squares)
    total = jnp.sum(total, axis=(0, 1), keepdims=True)
    sum_ref[...] = jnp.broadcast_to(total[:, None], sum_ref.shape)


def hold(x):
    return pltpu.with_memory_space_constraint(x, pltpu.VMEM)


def work(count):
    shapes = [(64, count, 128), (64, count, 128), (7 * 16, count, 128), (16, count, 128)]
    return [pltpu.VMEM(shape, jnp.float32) for shape in shapes]


def estimate(updates):
    return pl.CostEstimate(
        flops=updates * 400_000_000, transcendentals=0, bytes_accessed=updates * 1_000_000
    )


def opposite_rings(shift):
    count = lax.axis_size(SPACE)
    return [
        (core * count + i, core * count + (i + way) % count)
        for core, way in ((0, shift), (1, -shift))
        for i in range(count)
    ]


def ring(axis, shift):
    count = lax.axis_size(axis)
    return [(i, (i + shift) % count) for i in range(count)]


def on_device(slab_starts, coarse_factor, blend_weight, blend_flags):
    f32 = jnp.float32
    vmem = pl.BlockSpec(memory_space=pltpu.VMEM)
    smem = pl.BlockSpec(memory_space=pltpu.SMEM)
    opening = slab_starts.reshape(64, 8, 128)
    slab = lax.axis_index(TM).astype(jnp.int32).reshape(1)
    raw = pl.BlockSpec(memory_space=pl.ANY)
    own = pl.pallas_call(
        join_kernel,
        out_shape=pltpu.VMEM((65, 8, 128), f32),
        in_specs=[raw] * 3,
        out_specs=vmem,
        scratch_shapes=[
            pltpu.VMEM((8, 128), f32),
            pltpu.VMEM((8, 128), jnp.int32),
            pltpu.SemaphoreType.DMA((3,)),
        ],
        name="join",
    )(opening, blend_weight, blend_flags)
    factor = hold(coarse_factor)
    own = hold(own)
    first = hold(lax.ppermute(own, PLANE, opposite_rings(1)))
    inner = pl.pallas_call(
        inner_kernel,
        out_shape=pltpu.VMEM((3, 64, 8, 128), f32),
        in_specs=[vmem],
        out_specs=vmem,
        scratch_shapes=work(16),
        cost_estimate=estimate(3),
        name="inner",
    )(own)
    again, inner = lax.optimization_barrier((own, inner))
    block = hold(lax.ppermute(again, PLANE, opposite_rings(-1)))
    inner = hold(inner)
    strip = pl.pallas_call(
        strip_kernel,
        out_shape=pltpu.VMEM((64, 8, 128), f32),
        in_specs=[smem] + [vmem] * 3,
        out_specs=vmem,
        scratch_shapes=work(24) + [pltpu.VMEM((24, 128), f32)],
        cost_estimate=estimate(4),
        name="strip",
    )(slab, own, first, inner)
    sent, plain = pl.pallas_call(
        fine_kernel,
        out_shape=(
            pltpu.VMEM((32, 8, 128), f32),
            pltpu.VMEM((64, 8, 128), f32),
        ),
        in_specs=[smem] + [vmem] * 6,
        out_specs=[vmem] * 2,
        scratch_shapes=work(24) + [pltpu.VMEM((24, 128), f32)],
        cost_estimate=estimate(11),
        name="fine",
    )(slab, own, first, block, inner, hold(strip), factor)
    plain = hold(plain)
    got = hold(lax.ppermute(sent, TM[1], ring(TM[1], 1)))
    both = pl.pallas_call(
        pair_kernel,
        out_shape=pltpu.VMEM((8, 4, 8, 128), f32),
        in_specs=[smem] + [vmem] * 3,
        out_specs=vmem,
        name="pair",
    )(slab, plain, got, factor)
    gathered = lax.all_to_all(both, TM[0], 0, 0)
    scanned = pl.pallas_call(
        scan_kernel,
        out_shape=pltpu.VMEM((8, 4, 8, 128), f32),
        in_specs=[smem] + [vmem] * 2,
        out_specs=vmem,
        name="scan",
    )(slab, hold(gathered), factor)
    pieces = lax.all_to_all(scanned, TM[0], 0, 0)
    kept, given = pl.pallas_call(
        spread_kernel,
        out_shape=(pltpu.VMEM((32, 8, 128), f32), pltpu.VMEM((32, 8, 128), f32)),
        in_specs=[smem] + [vmem] * 4,
        out_specs=[vmem] * 2,
        name="spread",
    )(slab, hold(pieces), plain, got, factor)
    arrived = lax.ppermute(given, TM[1], ring(TM[1], 1))
    slab_end, partial_sums = pl.pallas_call(
        final_kernel,
        out_shape=(
            pltpu.VMEM((64, 8, 128), f32),
            pltpu.VMEM((16, 1, 128), f32),
        ),
        in_specs=[smem] + [vmem] * 5,
        out_specs=[vmem] * 2,
        scratch_shapes=[pltpu.VMEM((64, 8, 128), f32)],
        name="final",
    )(slab, hold(kept), hold(arrived), own, plain, factor)
    shared = lax.all_to_all(partial_sums, SPACE, 0, 0)
    element_count = lax.axis_size(SPACE) * slab_starts.shape[4] * slab_starts.shape[5]
    jump_norm = jnp.sqrt(jnp.sum(shared[:, 0, 0]) / element_count)
    return (slab_end.reshape(slab_starts.shape), jump_norm[None])


def solution(mesh):
    split = Mesh(mesh.devices.reshape(8, 2, 4, 4), ("tm_0", "tm_1", "space_0", "space_1"))
    return jax.shard_map(
        on_device,
        mesh=split,
        in_specs=(
            P(TM, None, None, None, SPACE, None),
            P(None, SPACE, None),
            P(SPACE, None),
            P(SPACE, None),
        ),
        out_specs=(P(TM, None, None, None, SPACE, None), P(TM)),
        check_vma=False,
    )
```

```python
import math

import jax
import jax.numpy as jnp
import numpy as np
from jax import lax
from jax.experimental import pallas as pl
from jax.experimental.pallas import tpu as pltpu
from jax.sharding import Mesh
from jax.sharding import PartitionSpec as P

FSTEPS = 4
SPACE = ("space_0", "space_1")
TM = ("tm_0", "tm_1")
PLANE = ("tm_1", "space_0", "space_1")
STEP = 0.003
WEIGHTS = (1.0 / 6.0, 5.0 / 6.0, 5.0 / 6.0, 1.0 / 6.0)


def derivative_table():
    inner = 1.0 / math.sqrt(5.0)
    points = np.array([-1.0, -inner, inner, 1.0])
    scales = np.array(
        [1.0 / np.prod([points[c] - points[o] for o in range(4) if o != c]) for c in range(4)]
    )
    table = np.zeros((4, 4))
    for r in range(4):
        for c in range(4):
            if r != c:
                table[r, c] = scales[c] / scales[r] / (points[r] - points[c])
        table[r, r] = -np.sum(table[r])
    return table


SPLIT = [[float(2.0 * WEIGHTS[i] * derivative_table()[i, k]) for k in range(4)] for i in range(4)]
EDGE = SPLIT[0][1]
SERIES = (105.0 / 52.5, 35.0 / 52.5, 21.0 / 52.5, 15.0 / 52.5)
BINARY = tuple(x / math.log(2.0) for x in SERIES)
BETA = 0.2 / math.log(2.0)
SOUND = math.sqrt(1.4 * BETA)


def log_parts(left, right, log_left, log_right, terms):
    total = left + right
    differ = right - left
    ratio = differ / total
    ratio = ratio * ratio
    nearly = ratio < 0.0001
    series = terms[0] + ratio * (terms[1] + ratio * (terms[2] + ratio * terms[3]))
    return jnp.where(nearly, total, differ), jnp.where(nearly, series, log_right - log_left)


def pair_flux(a, b, scale=None):
    top, bottom = log_parts(a["rho"], b["rho"], a["lrho"], b["lrho"], SERIES)
    mean = top / bottom
    top, bottom = log_parts(a["beta"], b["beta"], a["lbeta"], b["lbeta"], BINARY)
    thermal = bottom / top
    normal = a["n"] + b["n"]
    pressure = a["p"] + b["p"]
    cross = a["p"] * b["n"] + b["p"] * a["n"]
    if scale is not None:
        mean = mean * scale
        pressure = pressure * scale
        cross = cross * scale
    mass = mean * normal
    half = 0.5 * mass
    kinetic = a["n"] * b["n"] + a["t"] * b["t"] + thermal
    return (
        mass,
        half * normal + pressure,
        half * (a["t"] + b["t"]),
        half * kinetic + cross,
    )


def conserved(node):
    return (node["rho"], node["mn"], node["mt"], node["e"])


def face_flux(a, b, scale):
    central = pair_flux(a, b)
    speed = jnp.maximum(jnp.abs(a["n"]) + a["c"], jnp.abs(b["n"]) + b["c"])
    return tuple(
        scale * (c - speed * (ub - ua)) for c, ua, ub in zip(central, conserved(a), conserved(b), strict=True)
    )


def physical(node):
    return (
        node["mn"],
        node["mn"] * node["n"] + node["p"],
        node["mt"] * node["n"],
        node["n"] * (node["e"] + node["p"]),
    )


def line_walls(nodes, split_share, sub_share):
    pair = {}
    for i in range(4):
        for k in range(i + 1, 4):
            scale = None if k - i == 1 and i != 1 else SPLIT[i][k] / EDGE
            pair[i, k] = pair_flux(nodes[i], nodes[k], scale)
    own = [physical(node) for node in nodes]
    speeds = [jnp.abs(node["n"]) + node["c"] for node in nodes]
    out = [[], [], []]
    for v in range(4):
        far = pair[0, 3][v]
        left, right = far + pair[0, 2][v], far + pair[1, 3][v]
        walls = (
            left + pair[0, 1][v],
            (left + pair[1, 3][v]) + pair[1, 2][v],
            right + pair[2, 3][v],
        )
        for m in range(3):
            speed = jnp.maximum(speeds[m], speeds[m + 1])
            jump = conserved(nodes[m + 1])[v] - conserved(nodes[m])[v]
            sub = own[m][v] + own[m + 1][v] - speed * jump
            out[m].append(split_share * walls[m] + sub_share * sub)
    return out


ORDER = {1: (0, 1, 2, 3), 2: (0, 2, 1, 3)}
VX, VY, PR, LR, BE, LB, CS = range(7)


def at(v, i, j):
    return v * 16 + i * 4 + j


def rows(c, offset):
    start = c * 8 + offset
    if isinstance(c, int):
        return pl.ds(start, 8)
    return pl.ds(pl.multiple_of(c * 8, 8) + offset, 8)


def node_pass(src, prim, c):
    here = rows(c, 0)
    for n in range(16):
        rho = src[n, here, :]
        inv = 1.0 / rho
        mx = src[16 + n, here, :]
        my = src[32 + n, here, :]
        vx = mx * inv
        vy = my * inv
        p = 0.4 * src[48 + n, here, :] - 0.2 * (mx * vx + my * vy)
        beta = BETA * rho / p
        prim[VX * 16 + n, here, :] = vx
        prim[VY * 16 + n, here, :] = vy
        prim[PR * 16 + n, here, :] = p
        prim[LR * 16 + n, here, :] = jnp.log(rho)
        prim[BE * 16 + n, here, :] = beta
        prim[LB * 16 + n, here, :] = jnp.log2(beta)
        prim[CS * 16 + n, here, :] = SOUND * lax.rsqrt(beta)


def node(src, prim, i, j, here, axis):
    n = i * 4 + j
    normal, along = (VX, VY) if axis == 1 else (VY, VX)
    order = ORDER[axis]
    return {
        "rho": src[n, here, :],
        "mn": src[order[1] * 16 + n, here, :],
        "mt": src[order[2] * 16 + n, here, :],
        "e": src[48 + n, here, :],
        "n": prim[normal * 16 + n, here, :],
        "t": prim[along * 16 + n, here, :],
        "p": prim[PR * 16 + n, here, :],
        "lrho": prim[LR * 16 + n, here, :],
        "beta": prim[BE * 16 + n, here, :],
        "lbeta": prim[LB * 16 + n, here, :],
        "c": prim[CS * 16 + n, here, :],
    }


def face_pass(src, prim, faces, c, scale):
    for j in range(4):
        lower = node(src, prim, 3, j, rows(c, 0), 1)
        flux = face_flux(lower, node(src, prim, 0, j, rows(c, 1), 1), scale)
        for v in range(4):
            faces[j * 4 + v, rows(c, 0), :] = flux[v]


def update_pass(src, dst, prim, faces, c, blend, second, side):
    here = rows(c, 1)
    there, start_rows = rows(c, 2 * side), rows(c, 2 - 2 * side)
    scale = (0.5 if second else 1.0) * STEP / WEIGHTS[1]
    sub_share = scale * blend
    split_share = (scale - sub_share) * EDGE
    for j in range(4):
        nodes = [node(src, prim, i, j, here, 1) for i in range(4)]
        walls = line_walls(nodes, split_share, sub_share)
        for v in range(4):
            column = [faces[j * 4 + v, rows(c, 0), :]]
            column += [walls[m][v] for m in range(3)]
            column += [faces[j * 4 + v, here, :]]
            for i in range(4):
                k = at(v, i, j)
                change = column[i + 1] - column[i]
                if i in (0, 3):
                    change = (WEIGHTS[1] / WEIGHTS[0]) * change
                if second:
                    start = 0.5 * (dst[k, start_rows, :] + src[k, here, :])
                else:
                    start = src[k, here, :]
                dst[k, there, :] = start - change
    for i in range(4):
        nodes = [node(src, prim, i, j, here, 2) for j in range(4)]
        behind = {key: pltpu.roll(x, 1, 1) for key, x in nodes[3].items()}
        low = face_flux(behind, nodes[0], scale)
        high = tuple(pltpu.roll(x, 127, 1) for x in low)
        walls = line_walls(nodes, split_share, sub_share)
        for q in range(4):
            v = ORDER[2][q]
            column = [low[q]] + [walls[m][q] for m in range(3)] + [high[q]]
            for j in range(4):
                k = at(v, i, j)
                change = column[j + 1] - column[j]
                if j in (0, 3):
                    change = (WEIGHTS[1] / WEIGHTS[0]) * change
                dst[k, there, :] = dst[k, there, :] - change


def loop(count, body):
    if isinstance(count, int) and count == 1:
        body(0)
        return

    def step(c, carry):
        body(c)
        return carry

    lax.fori_loop(0, count, step, 0)


def stage(src, dst, work, second, side, chunks, blend_at, updates):
    prim, faces = work
    scale = (0.5 if second else 1.0) * STEP / WEIGHTS[1]
    loop(chunks, lambda c: node_pass(src, prim, c))
    loop(chunks, lambda c: face_pass(src, prim, faces, c, scale))
    loop(
        updates, lambda c: update_pass(src, dst, prim, faces, c, blend_at(c), second, side)
    )


def join_kernel(opening_ref, weight_ref, flags_ref, own_ref, weight, flags, sems):
    copies = [
        pltpu.make_async_copy(opening_ref, own_ref.at[pl.ds(0, 64)], sems.at[0]),
        pltpu.make_async_copy(weight_ref, weight, sems.at[1]),
        pltpu.make_async_copy(flags_ref, flags, sems.at[2]),
    ]
    for copy in copies:
        copy.start()
    copies[1].wait()
    copies[2].wait()
    own_ref[64] = flags[...].astype(jnp.float32) * weight[...]
    copies[0].wait()


def inner_kernel(own_ref, inner_ref, base, mid, prim, faces):
    for k in range(64):
        base[k, 0:8, :] = own_ref[k]
    blend = own_ref[64]
    for s in range(1, 4):
        second = s == 2
        src, dst = (mid, base) if second else (base, mid)
        shifted = pltpu.roll(blend, 8 - s, 0)
        stage(src, dst, (prim, faces), second, 0, 1, lambda c: shifted, 1)
        for k in range(64):
            inner_ref[s - 1, k] = dst[k, 0:8, :]


def begin_strip(base, own_ref, block_ref, side):
    for k in range(64):
        base[k, pl.ds(2 * side, 8), :] = block_ref[k]
        base[k, pl.ds(8 - 8 * side, 2), :] = own_ref[k, pl.ds(6 * side, 2), :]


def continue_strip(dst, inner_ref, s, side):
    def one(k, carry):
        dst[k, pl.ds(8 - 8 * side, 2), :] = inner_ref[s - 1, k, pl.ds(side * (6 - 2 * s), 2), :]
        return carry

    lax.fori_loop(0, 64, one, 0, unroll=16)


def strip_kernel(
    slab_ref, own_ref, block_ref, inner_ref, out_ref, base, mid, prim, faces, blend_ref
):
    side = slab_ref[0] & 1
    begin_strip(base, own_ref, block_ref, side)
    blend_ref[0:8, :] = block_ref[64]
    blend_ref[8:16, :] = own_ref[64]
    blend_ref[16:24, :] = block_ref[64]

    def time_step(t, carry):
        for second in (False, True):
            s = 2 * t + (2 if second else 1)
            src, dst = (mid, base) if second else (base, mid)
            blend_at = lambda c, s=s: blend_ref[pl.ds(s + side * (16 - 2 * s), 8), :]
            stage(src, dst, (prim, faces), second, side, 2, blend_at, 1)
            continue_strip(dst, inner_ref, jnp.minimum(s, 3), side)
        return carry

    lax.fori_loop(0, 2, time_step, 0)
    for k in range(64):
        out_ref[k] = base[k, pl.ds(2 * side, 8), :]


def fine_kernel(
    slab_ref, own_ref, first_ref, block_ref, inner_ref, strip_ref, factor_ref,
    sent_ref, plain_ref, base, mid, prim, faces, blend_ref,
):
    other_side = slab_ref[0] & 1
    side = 1 - other_side
    begin_strip(base, own_ref, block_ref, side)
    blend_ref[pl.ds(16 * other_side, 8), :] = first_ref[64]
    blend_ref[8:16, :] = own_ref[64]
    blend_ref[pl.ds(16 * side, 8), :] = block_ref[64]

    def strip_step(t, carry):
        for second in (False, True):
            s = 2 * t + (2 if second else 1)
            src, dst = (mid, base) if second else (base, mid)
            blend_at = lambda c, s=s: blend_ref[pl.ds(s + side * (16 - 2 * s), 8), :]
            stage(src, dst, (prim, faces), second, side, 2, blend_at, 1)
            continue_strip(dst, inner_ref, jnp.minimum(s, 3), side)
        return carry

    lax.fori_loop(0, 2, strip_step, 0)

    def merge(k, carry):
        strip = base[k, pl.ds(2 * side, 8), :]
        base[k, pl.ds(pl.multiple_of(8 * side, 8), 8), :] = strip
        base[k, pl.ds(pl.multiple_of(8 - 8 * side, 8), 8), :] = strip_ref[k]
        return carry

    lax.fori_loop(0, 64, merge, 0, unroll=16)

    def joint_step(t, carry):
        for second in (False, True):
            s = 2 * t + (2 if second else 1)
            src, dst = (mid, base) if second else (base, mid)
            blend_at = lambda c, s=s: blend_ref[pl.ds(8 * c + s, 8), :]
            updates = jnp.where(s < 8, 2, 1) if second else 2
            stage(src, dst, (prim, faces), second, 0, 2, blend_at, updates)
        return carry

    lax.fori_loop(2, FSTEPS, joint_step, 0)

    later = jnp.where(slab_ref[0] == 0, 0.0, 1.0).astype(jnp.float32)
    for v in range(4):
        factor = factor_ref[v]
        mean = weighted_mean([own_ref[v * 16 + n] for n in range(16)])
        for n in range(16):
            k = v * 16 + n
            guess = mean + factor * (own_ref[k] - mean)
            plain_ref[k] = base[k, 0:8, :] - later * guess
    other = 32 * (1 - (slab_ref[0] & 1))
    for k in range(32):
        sent_ref[k] = plain_ref[other + k]


def weighted_mean(values):
    total = None
    for n, x in enumerate(values):
        term = (WEIGHTS[n // 4] * WEIGHTS[n % 4] / 4.0) * x
        total = term if total is None else total + term
    return total


def exchange(blocks):
    group = lax.broadcasted_iota(jnp.int32, (8, 128), 0) // 2
    out = []
    for q in range(4):
        piece = None
        for j in range(4):
            shift = (2 * (j - q)) % 8
            moved = pltpu.roll(blocks[j], shift, 0) if shift else blocks[j]
            piece = moved if piece is None else jnp.where(group == j, moved, piece)
        out.append(piece)
    return out


def chip_parts(slab_ref, plain_ref, got_ref, w):
    core = slab_ref[0] & 1
    even_here = core == 0
    evens, odds = [], []
    for n in range(16):
        mine, theirs = plain_ref[32 * core + 16 * w + n], got_ref[16 * w + n]
        evens.append(jnp.where(even_here, mine, theirs))
        odds.append(jnp.where(even_here, theirs, mine))
    return core, evens, odds


def pair_kernel(slab_ref, plain_ref, got_ref, factor_ref, out_ref):
    for w in range(2):
        core, evens, odds = chip_parts(slab_ref, plain_ref, got_ref, w)
        factor = factor_ref[2 * core + w]
        mean = weighted_mean(evens)
        both = [mean + factor * (x - mean) + y for x, y in zip(evens, odds, strict=True)]
        for i in range(4):
            for q, piece in enumerate(exchange(both[4 * i : 4 * i + 4])):
                out_ref[w * 4 + q, i] = piece


def scan_kernel(slab_ref, given_ref, factor_ref, out_ref):
    slab = slab_ref[0]
    chip = lax.shift_right_logical(slab, 1)
    var = 2 * (slab & 1) + lax.shift_right_logical(chip, 2)
    first = 2 * (chip & 3)
    row = lax.broadcasted_iota(jnp.int32, (8, 128), 0)
    even = jnp.broadcast_to(factor_ref[var, pl.ds(first, 1), :], (8, 128))
    odd = jnp.broadcast_to(factor_ref[var, pl.ds(first + 1, 1), :], (8, 128))
    factor = jnp.where((row & 1) == 0, even, odd)
    factor = factor * factor
    outer = (row < 2) | (row >= 6)
    low = jnp.where(outer, WEIGHTS[0], WEIGHTS[1]).astype(jnp.float32) * (WEIGHTS[0] / 4.0)
    high = jnp.where(outer, WEIGHTS[0], WEIGHTS[1]).astype(jnp.float32) * (WEIGHTS[1] / 4.0)
    state = [given_ref[0, i] for i in range(4)]
    for i in range(4):
        out_ref[0, i] = state[i]
    for n in range(1, 8):
        for i in range(4):
            out_ref[n, i] = state[i]
        if n == 7:
            break
        part = (state[0] + state[3]) * low + (state[1] + state[2]) * high
        part = part + pltpu.roll(part, 4, 0)
        mean = part + pltpu.roll(part, 2, 0)
        state = [mean + factor * (state[i] - mean) + given_ref[n, i] for i in range(4)]


def spread_kernel(slab_ref, pieces_ref, plain_ref, got_ref, factor_ref, kept_ref, sent_ref):
    later = jnp.where(slab_ref[0] < 2, 0.0, 1.0).astype(jnp.float32)
    for w in range(2):
        core, evens, _ = chip_parts(slab_ref, plain_ref, got_ref, w)
        factor = factor_ref[2 * core + w]
        starts = []
        for i in range(4):
            starts += exchange([pieces_ref[w * 4 + q, i] for q in range(4)])
        mean = weighted_mean(starts)
        for n in range(16):
            second = later * (mean + factor * (starts[n] - mean)) + evens[n]
            kept_ref[16 * w + n] = jnp.where(core == 0, starts[n], second)
            sent_ref[16 * w + n] = jnp.where(core == 0, second, starts[n])


def final_kernel(
    slab_ref, kept_ref, got_ref, own_ref, plain_ref, factor_ref, end_ref, sum_ref, starts_ref
):
    later = jnp.where(slab_ref[0] == 0, 0.0, 1.0).astype(jnp.float32)
    here = 32 * (slab_ref[0] & 1)
    for k in range(32):
        starts_ref[here + k] = kept_ref[k]
        starts_ref[32 - here + k] = got_ref[k]
    total = jnp.zeros((8, 128), jnp.float32)
    for v in range(4):
        factor = factor_ref[v]
        starts = [starts_ref[v * 16 + n] for n in range(16)]
        mean = weighted_mean(starts)
        squares = []
        for n in range(16):
            k = v * 16 + n
            end_ref[k] = later * (mean + factor * (starts[n] - mean)) + plain_ref[k]
            jump = later * (starts[n] - own_ref[k])
            squares.append(jump * jump)
        total = total + weighted_mean(squares)
    total = jnp.sum(total, axis=(0, 1), keepdims=True)
    sum_ref[...] = jnp.broadcast_to(total[:, None], sum_ref.shape)


def hold(x):
    return pltpu.with_memory_space_constraint(x, pltpu.VMEM)


def work(count):
    shapes = [(64, count, 128), (64, count, 128), (7 * 16, count, 128), (16, count, 128)]
    return [pltpu.VMEM(shape, jnp.float32) for shape in shapes]


def estimate(updates):
    return pl.CostEstimate(
        flops=updates * 400_000_000, transcendentals=0, bytes_accessed=updates * 1_000_000
    )


def opposite_rings(shift):
    count = lax.axis_size(SPACE)
    return [
        (core * count + i, core * count + (i + way) % count)
        for core, way in ((0, shift), (1, -shift))
        for i in range(count)
    ]


def ring(axis, shift):
    count = lax.axis_size(axis)
    return [(i, (i + shift) % count) for i in range(count)]


def on_device(slab_starts, coarse_factor, blend_weight, blend_flags):
    f32 = jnp.float32
    vmem = pl.BlockSpec(memory_space=pltpu.VMEM)
    smem = pl.BlockSpec(memory_space=pltpu.SMEM)
    opening = slab_starts.reshape(64, 8, 128)
    slab = lax.axis_index(TM).astype(jnp.int32).reshape(1)
    raw = pl.BlockSpec(memory_space=pl.ANY)
    own = pl.pallas_call(
        join_kernel,
        out_shape=pltpu.VMEM((65, 8, 128), f32),
        in_specs=[raw] * 3,
        out_specs=vmem,
        scratch_shapes=[
            pltpu.VMEM((8, 128), f32),
            pltpu.VMEM((8, 128), jnp.int32),
            pltpu.SemaphoreType.DMA((3,)),
        ],
        name="join",
    )(opening, blend_weight, blend_flags)
    factor = hold(coarse_factor)
    own = hold(own)
    first = hold(lax.ppermute(own, PLANE, opposite_rings(1)))
    inner = pl.pallas_call(
        inner_kernel,
        out_shape=pltpu.VMEM((3, 64, 8, 128), f32),
        in_specs=[vmem],
        out_specs=vmem,
        scratch_shapes=work(16),
        cost_estimate=estimate(3),
        name="inner",
    )(own)
    again, inner = lax.optimization_barrier((own, inner))
    block = hold(lax.ppermute(again, PLANE, opposite_rings(-1)))
    inner = hold(inner)
    strip = pl.pallas_call(
        strip_kernel,
        out_shape=pltpu.VMEM((64, 8, 128), f32),
        in_specs=[smem] + [vmem] * 3,
        out_specs=vmem,
        scratch_shapes=work(24) + [pltpu.VMEM((24, 128), f32)],
        cost_estimate=estimate(4),
        name="strip",
    )(slab, own, first, inner)
    sent, plain = pl.pallas_call(
        fine_kernel,
        out_shape=(
            pltpu.VMEM((32, 8, 128), f32),
            pltpu.VMEM((64, 8, 128), f32),
        ),
        in_specs=[smem] + [vmem] * 6,
        out_specs=[vmem] * 2,
        scratch_shapes=work(24) + [pltpu.VMEM((24, 128), f32)],
        cost_estimate=estimate(11),
        name="fine",
    )(slab, own, first, block, inner, hold(strip), factor)
    plain = hold(plain)
    got = hold(lax.ppermute(sent, TM[1], ring(TM[1], 1)))
    both = pl.pallas_call(
        pair_kernel,
        out_shape=pltpu.VMEM((8, 4, 8, 128), f32),
        in_specs=[smem] + [vmem] * 3,
        out_specs=vmem,
        name="pair",
    )(slab, plain, got, factor)
    gathered = lax.all_to_all(both, TM[0], 0, 0)
    scanned = pl.pallas_call(
        scan_kernel,
        out_shape=pltpu.VMEM((8, 4, 8, 128), f32),
        in_specs=[smem] + [vmem] * 2,
        out_specs=vmem,
        name="scan",
    )(slab, hold(gathered), factor)
    pieces = lax.all_to_all(scanned, TM[0], 0, 0)
    kept, given = pl.pallas_call(
        spread_kernel,
        out_shape=(pltpu.VMEM((32, 8, 128), f32), pltpu.VMEM((32, 8, 128), f32)),
        in_specs=[smem] + [vmem] * 4,
        out_specs=[vmem] * 2,
        name="spread",
    )(slab, hold(pieces), plain, got, factor)
    arrived = lax.ppermute(given, TM[1], ring(TM[1], 1))
    slab_end, partial_sums = pl.pallas_call(
        final_kernel,
        out_shape=(
            pltpu.VMEM((64, 8, 128), f32),
            pltpu.VMEM((16, 1, 128), f32),
        ),
        in_specs=[smem] + [vmem] * 5,
        out_specs=[vmem] * 2,
        scratch_shapes=[pltpu.VMEM((64, 8, 128), f32)],
        name="final",
    )(slab, hold(kept), hold(arrived), own, plain, factor)
    shared = lax.all_to_all(partial_sums, SPACE, 0, 0)
    element_count = lax.axis_size(SPACE) * slab_starts.shape[4] * slab_starts.shape[5]
    jump_norm = jnp.sqrt(jnp.sum(shared[:, 0, 0]) / element_count)
    return (slab_end.reshape(slab_starts.shape), jump_norm[None])


def solution(mesh):
    split = Mesh(mesh.devices.reshape(8, 2, 4, 4), ("tm_0", "tm_1", "space_0", "space_1"))
    return jax.shard_map(
        on_device,
        mesh=split,
        in_specs=(
            P(TM, None, None, None, SPACE, None),
            P(None, SPACE, None),
            P(SPACE, None),
            P(SPACE, None),
        ),
        out_specs=(P(TM, None, None, None, SPACE, None), P(TM)),
        check_vma=False,
    )
```
